128 devices in a mesh: leaf: 128 (over z, x, y, core).
Axes of the slice: x: 4, y: 4, z: 4, core: 2. Of those that a mesh axis runs over, the one named last changes fastest.
Arguments:
- coords: float32 [3, 1048576], P(None, 'leaf'), may hold values from 0 to 1
- charges: bfloat16 [1048576, 128], P('leaf'), may hold values from -6 to 6
- near_leaves: int32 [8192, 27], P('leaf'), may hold values from 0 to 191
- leaf_basis: bfloat16 [8192, 4096], P('leaf'), may hold values from -1 to 1
- leaf_transfer: bfloat16 [8192, 1024], P('leaf'), may hold values from -0.75 to 0.75
- mid_transfer: bfloat16 [1024, 1024], P('leaf'), may hold values from -0.75 to 0.75
- base_transfer: bfloat16 [128, 1024], P('leaf'), may hold values from -0.75 to 0.75
- base_coupling: bfloat16 [24192, 1024], P('leaf'), may hold values from -0.01953125 to 0.01953125
- base_target: int32 [24192, 1], P('leaf'), may hold values from 0 to 127; in each aligned block of 189 rows (0 to 188, 189 to 377, ...) at most 2 rows name the same one
- base_source: int32 [24192], P('leaf'), may hold values from 0 to 127
- top_coupling: bfloat16 [1024, 1024], P('leaf'), may hold values from -0.015625 to 0.015625
- top_target: int32 [1024], P('leaf'), may hold values from 0 to 15
- top_source: int32 [1024], P('leaf'), may hold values from 0 to 15
Outputs:
- potential: bfloat16 [1048576, 128], P('leaf')
The draws below stay inside these ranges and needn't reach their ends.
Inputs may be any that keep to these rules, and one draw needn't show every extreme that they name: `near_leaves`: entry j of leaf l names leaf 64 * (l // 64 - 1) + j: a leaf of the device before in Morton order, of the row's own device, or of the device after; repeats may occur. `base_target`: among the 189 blocks of one device no base cluster is the target more than 2 times; that count is reached.
All inputs are finite; a program needn't handle non-finite values.
Results may differ from the reference program's by a relative error of at most 0.01.
Values may be sent and summed in bfloat16 or wider, within the bound.
No kernel may reach another device: no remote copies, remote signals or barrier semaphores. Data moves between devices by JAX's collectives and lax.ppermute only.
A program may use at most 128 MiB of HBM per device.

```python
import math
import jax
import jax.numpy as jnp
import numpy as np
from jax import lax

K = 32
RHS = 128
M = 128
NNEAR = 27
NB = 189
TOPB_DEV = 8
LEAF_DEV = 64
BASE_DEV = 1
LEAVES = 8192
NPTS = 1048576
MIDS = 1024
NBASE = 128
NTOP = 16
BLK_DEV = 189
NBLK = 24192
NTBLK = 1024
CAPC = 2
N_LEAF = 128


def set_ends(drawn, stream_key, smallest, top_value):
    shape = drawn.shape
    spot = [jax.random.randint(jax.random.fold_in(stream_key, axis), (), 0, shape[axis]) for axis in range(len(shape))]
    drawn = drawn.at[tuple(spot)].set(smallest)
    longest = shape.index(max(shape))
    spot[longest] = (spot[longest] + 1) % shape[longest]
    return drawn.at[tuple(spot)].set(top_value)


def shard_levels(rng, dims, pieces, smallest, high):
    loudness, own = 1.0, jax.random.fold_in(rng, 6)
    for position, blocks in pieces:
        draws = jnp.exp(jax.random.uniform(jax.random.fold_in(own, position), (blocks,), jnp.float32, smallest / len(pieces), high / len(pieces)))
        loudness = loudness * jnp.repeat(draws, dims[position] // blocks).reshape([-1 if axis == position else 1 for axis in range(len(dims))])
    return loudness


def shared_out(rng, own, number, rows, amount, top, bound, slope):
    ranking = jax.random.permutation(rng, amount)
    heavy_load, ordinary = shares(amount, rows * top, bound, slope, True), shares(amount, rows * top, bound, slope, False)
    places = jnp.arange(amount)

    def named(lengths, offset_by):
        used = int((lengths > 0).sum())
        fixed = max(1, used // 4)
        passed = fixed + (places - fixed + offset_by * (used - fixed)) % max(1, amount - fixed)
        return jnp.zeros((amount,), jnp.int32).at[ranking[jnp.where(places < fixed, places, passed)]].set(jnp.asarray(lengths, jnp.int32))

    lengths = jnp.where(number % 4 == 0, named(heavy_load, number // 4), named(ordinary, number - number // 4 - 1))
    mixed = jax.random.permutation(jax.random.fold_in(own, 3), amount)
    source_of, taker = mixed[0:amount // 2 * 2:2], mixed[1:amount // 2 * 2:2]
    margin = jnp.minimum(lengths[source_of] - 1, bound - lengths[taker]) // 2
    margin = jnp.where((source_of == ranking[0]) | (taker == ranking[0]) | (lengths[taker] == 0), 0, jnp.maximum(margin, 0))
    passed = jax.random.randint(jax.random.fold_in(own, 4), (amount // 2,), 0, 1 << 20) % (margin + 1)
    lengths = lengths.at[source_of].add(-passed).at[taker].add(passed)
    labels = jnp.searchsorted(jnp.cumsum(lengths), jnp.arange(rows * top), side="right").astype(jnp.int32)
    listing = labels.reshape(top, rows).T
    listing = listing[jax.random.permutation(jax.random.fold_in(own, 1), rows)]
    offset_by = jax.random.randint(jax.random.fold_in(own, 2), (rows, 1), 0, top)
    return jnp.take_along_axis(listing, (jnp.arange(top)[None, :] + offset_by) % top, axis=1)


def shares(count, total, bound, lean, full):
    weights = [(1 << 20) // math.isqrt(grade ** lean) + 1 for grade in range(1, count + 1)]
    largest = bound if full else min(bound, max(-(-total // count), total * weights[0] // sum(weights)))
    least = 1 if total - largest >= count - 1 else 0
    counts, spare = [largest] + [least] * (count - 1), total - largest - least * (count - 1)
    while spare > 0:
        movable = [i for i in range(1, count) if counts[i] < largest] or [i for i in range(1, count) if counts[i] < bound]
        whole, remaining = sum([weights[i] for i in movable]), spare
        for i in movable:
            more = min(bound - counts[i], max(1, remaining * weights[i] // whole), spare)
            counts[i] = counts[i] + more
            spare = spare - more
    return np.array(counts)


def centred(key, dims, spread, bound, pieces=(), kind=jnp.bfloat16):
    result = spread * jax.random.normal(key, dims, jnp.float32)
    if pieces:
        result = result * shard_levels(key, dims, pieces, -0.22, 0.18)
    return jnp.clip(result, -bound, bound).astype(kind)


def setup_inputs(seed: int = 0) -> dict:
    arg_keys = jax.random.split(jax.random.key(seed), 14)
    coords = jnp.clip(1.0 * jax.random.uniform(arg_keys[0], (3, NPTS), jnp.float32) ** shard_levels(arg_keys[0], (3, NPTS), ((1, 128),), -0.2, 0.2), 0.0, 1.0)
    charges = centred(arg_keys[1], (NPTS, RHS), 1.0, 6.0, ((0, 128),))
    near_leaves = set_ends(jax.random.randint(arg_keys[2], (LEAVES, NNEAR), 0, 3 * LEAF_DEV), jax.random.fold_in(arg_keys[2], 1), 0, (3 * LEAF_DEV) - 1).astype(jnp.int32)
    leaf_basis = centred(arg_keys[3], (LEAVES, K * M), K ** -0.5, 1.0, ((0, 128),))
    leaf_transfer = centred(arg_keys[4], (LEAVES, K * K), (2 * K) ** -0.5, 0.75, ((0, 128),))
    mid_transfer = centred(arg_keys[5], (MIDS, K * K), (2 * K) ** -0.5, 0.75, ((0, 128),))
    base_transfer = centred(arg_keys[6], (NBASE, K * K), (2 * K) ** -0.5, 0.75, ((0, 128),))
    base_coupling = centred(arg_keys[7], (NBLK, K * K), (16 * K * NB) ** -0.5, 0.01953125, ((0, 128),))
    base_target_keys = jax.random.split(jax.random.fold_in(arg_keys[8], 1), NBLK // BLK_DEV)
    base_target_turns = jax.random.permutation(jax.random.fold_in(arg_keys[8], 3), NBLK // BLK_DEV)
    base_target = jax.vmap(lambda own, number: shared_out(jax.random.fold_in(arg_keys[8], 2), own, number, BLK_DEV, NBASE, 1, CAPC, 1))(base_target_keys, base_target_turns).reshape((NBLK, 1))
    base_source = set_ends(jax.random.randint(arg_keys[9], (NBLK,), 0, NBASE), jax.random.fold_in(arg_keys[9], 1), 0, NBASE - 1).astype(jnp.int32)
    top_coupling = centred(arg_keys[10], (NTBLK, K * K), (512 * K * TOPB_DEV // BASE_DEV) ** -0.5, 0.015625, ((0, 128),))
    top_target = set_ends(jax.random.randint(arg_keys[11], (NTBLK,), 0, NTOP), jax.random.fold_in(arg_keys[11], 1), 0, NTOP - 1).astype(jnp.int32)
    top_source = set_ends(jax.random.randint(arg_keys[12], (NTBLK,), 0, NTOP), jax.random.fold_in(arg_keys[12], 1), 0, NTOP - 1).astype(jnp.int32)
    return {"coords": coords, "charges": charges, "near_leaves": near_leaves, "leaf_basis": leaf_basis, "leaf_transfer": leaf_transfer, "mid_transfer": mid_transfer, "base_transfer": base_transfer, "base_coupling": base_coupling, "base_target": base_target, "base_source": base_source, "top_coupling": top_coupling, "top_target": top_target, "top_source": top_source}


delta_sq = 0.0025

def rounded_values(values):
    return lax.optimization_barrier(values.astype(jnp.bfloat16))

def near_block(points, pool_points, pool_charges, columns):
    near_scale = 1.0 / math.sqrt(columns.shape[1] * points.shape[2])

    def near_step(running, column):
        other_points = jnp.take(pool_points, column, axis=1)
        other_charges = jnp.take(pool_charges, column, axis=0)
        squares = lax.optimization_barrier(jnp.sum((points[:, :, :, None] - other_points[:, :, None, :]) ** 2, axis=0))
        kernel = rounded_values(near_scale / jnp.sqrt(squares + delta_sq))
        update = jnp.einsum('lab,lbr->lar', kernel.astype(jnp.float32), other_charges.astype(jnp.float32))
        return (running + update, None)
    initial = jnp.zeros((points.shape[1], points.shape[2], pool_charges.shape[2]), jnp.float32)
    running, unused = lax.scan(near_step, initial, columns.T)
    return running

def reference(coords, charges, near_leaves, leaf_basis, leaf_transfer, mid_transfer, base_transfer, base_coupling, base_target, base_source, top_coupling, top_target, top_source):
    single_precision = jnp.float32
    charge_row_block = charges.reshape(LEAVES, M, RHS)
    basis_matrix = leaf_basis.reshape(LEAVES, K, M)
    leaf_coefficients = rounded_values(jnp.einsum('xpt,xtu->xpu', basis_matrix.astype(single_precision), charge_row_block.astype(single_precision)))
    mid_coeffs = rounded_values(jnp.einsum('mckp,mckr->mpr', leaf_transfer.reshape(MIDS, 8, K, K).astype(single_precision), leaf_coefficients.reshape(MIDS, 8, K, RHS).astype(single_precision)))
    base_coeffs = rounded_values(jnp.einsum('mckp,mckr->mpr', mid_transfer.reshape(NBASE, 8, K, K).astype(single_precision), mid_coeffs.reshape(NBASE, 8, K, RHS).astype(single_precision)))
    base_lift = base_transfer.reshape(NBASE, K, K)
    lifted = rounded_values(jnp.einsum('bkp,bkr->bpr', base_lift.astype(single_precision), base_coeffs.astype(single_precision)))
    top_coeffs = rounded_values(lax.optimization_barrier(jnp.sum(lifted.reshape(NTOP, 8, K, RHS).astype(single_precision), axis=1)))

    def add_portion(running, portion):
        blocks, targets, sources = portion
        products = jnp.einsum('bts,bsr->btr', blocks.reshape(-1, K, K).astype(single_precision), jnp.take(base_coeffs, sources, axis=0).astype(single_precision))
        return (running + jax.ops.segment_sum(products, targets, num_segments=NBASE), None)
    portions = (base_coupling.reshape(N_LEAF, BLK_DEV, K * K), base_target.reshape(N_LEAF, BLK_DEV), base_source.reshape(N_LEAF, BLK_DEV))
    coupled, unused = lax.scan(add_portion, jnp.zeros((NBASE, K, RHS), single_precision), portions)
    top_products = jnp.einsum('bts,bsr->btr', top_coupling.reshape(NTBLK, K, K).astype(single_precision), jnp.take(top_coeffs, top_source, axis=0).astype(single_precision))
    top_field = rounded_values(jax.ops.segment_sum(top_products, top_target, num_segments=NTOP))
    base_field = rounded_values(coupled + jnp.einsum('bkp,bpr->bkr', base_lift.astype(single_precision), jnp.repeat(top_field, 8, axis=0).astype(single_precision)))
    mid_field = rounded_values(jnp.einsum('mkp,mpr->mkr', mid_transfer.reshape(MIDS, K, K).astype(single_precision), jnp.repeat(base_field, 8, axis=0).astype(single_precision)))
    leaf_potential = rounded_values(jnp.einsum('lkp,lpr->lkr', leaf_transfer.reshape(LEAVES, K, K).astype(single_precision), jnp.repeat(mid_field, 8, axis=0).astype(single_precision)))
    all_points = coords.reshape(3, LEAVES, M)
    padded_points = jnp.pad(all_points, ((0, 0), (LEAF_DEV, LEAF_DEV), (0, 0)))
    padded_charges = jnp.pad(charge_row_block, ((LEAF_DEV, LEAF_DEV), (0, 0), (0, 0)))
    device_ids = jnp.arange(N_LEAF, dtype=jnp.int32)

    def device_block(portion):
        device, columns, local_expansion_basis, local_potential = portion
        first = (device * LEAF_DEV).astype(jnp.int32)
        points = lax.dynamic_slice_in_dim(all_points, first, LEAF_DEV, 1)
        pool_points = lax.dynamic_slice_in_dim(padded_points, first, 3 * LEAF_DEV, 1)
        pool_charges = lax.dynamic_slice_in_dim(padded_charges, first, 3 * LEAF_DEV, 0)
        near_field = near_block(points, pool_points, pool_charges, columns)
        distant_field = jnp.einsum('cbz,cbw->czw', local_expansion_basis.astype(single_precision), local_potential.astype(single_precision))
        return (near_field + distant_field).astype(jnp.bfloat16)
    inputs = (device_ids, near_leaves.reshape(N_LEAF, LEAF_DEV, NNEAR), basis_matrix.reshape(N_LEAF, LEAF_DEV, K, M), leaf_potential.reshape(N_LEAF, LEAF_DEV, K, RHS))
    potential = lax.map(device_block, inputs)
    return potential.reshape(NPTS, RHS)
```

```python
import math

import jax
import jax.numpy as jnp
from jax import lax
from jax.experimental import pallas as pl
from jax.experimental.pallas import tpu as pltpu
from jax.sharding import Mesh
from jax.sharding import PartitionSpec as P

K = 32
RHS = 128
M = 128
NNEAR = 27
LEAVES_DEV = 64
MIDS_DEV = 8
NBASE = 128
NTOP = 16
BLK_DEV = 189
BLK_PAD = 192
TOPB_DEV = 8
FEAT = 48
MSG = 48
LEAF = ("leaf_0", "leaf_1", "leaf_2", "leaf_3")
delta_sq = 0.0025
near_scale_sq = float(NNEAR * M)

f32 = jnp.float32
bf16 = jnp.bfloat16


def in_vmem():
    return pl.BlockSpec(memory_space=pltpu.VMEM)


def in_smem():
    return pl.BlockSpec(memory_space=pltpu.SMEM)


def in_place():
    return pl.BlockSpec(memory_space=pl.ANY)


def stacked_groups(tile):
    tile = tile.astype(f32)
    group = lax.broadcasted_iota(jnp.int32, tile.shape, 1) // K
    return jnp.concatenate([jnp.where(group == g, tile, 0.0) for g in range(4)], axis=0)


def rolled_groups(tile):
    tile = tile.astype(f32)
    lane = lax.broadcasted_iota(jnp.int32, tile.shape, 1)
    parts = [tile] + [pltpu.roll(tile, 128 - K * g, 1) for g in range(1, 4)]
    return jnp.concatenate([jnp.where(lane < K, part, 0.0) for part in parts], axis=0)


def unpermute(rows):
    to = lax.broadcasted_iota(jnp.int32, (K, K), 0)
    at = lax.broadcasted_iota(jnp.int32, (K, K), 1)
    order = jnp.where(to == 4 * (at % 8) + at // 8, 1.0, 0.0).astype(bf16)
    return jnp.dot(order, rows.astype(bf16), preferred_element_type=f32).astype(bf16)


def four_times(rows):
    return jnp.concatenate([rows] * 4, axis=0)


def up_kernel(q, basis, leaf_tiles, mid_tiles, lift_tile, lift_tile_t, message, vt):
    coeffs = jnp.zeros((K, RHS), f32)
    for m in range(MIDS_DEV):
        mid = four_times(unpermute(rolled_groups(mid_tiles[m])))
        lhs = jnp.concatenate([stacked_groups(leaf_tiles[8 * m + c]) for c in range(8)], axis=0)
        through = jnp.dot(lhs.astype(bf16), mid, preferred_element_type=f32)
        rows = []
        for c in range(8):
            turned = through[K * c : K * (c + 1)].T[:K].astype(bf16)
            v = jnp.dot(turned, basis[8 * m + c], preferred_element_type=f32).astype(bf16)
            vt[8 * m + c] = v
            rows.append(v)
        charges = q[pl.ds(8 * m, 8)].reshape(8 * M, RHS)
        coeffs = coeffs + jnp.dot(
            jnp.concatenate(rows, axis=1), charges, preferred_element_type=f32
        )
    whole = jnp.concatenate([coeffs, lift_tile[...].astype(f32), lift_tile_t[...].astype(f32)], axis=0)
    whole = whole.astype(bf16)

    def put(d, carry):
        message[d] = whole
        return carry

    lax.fori_loop(0, NBASE, put, 0, unroll=8)


def couple_kernel(
    first, second, sources, top_target, top_source, gathered, tiles, top_tiles, out, top_sum, top_rows
):
    top_sum[...] = jnp.zeros((NTOP, K, RHS), f32)
    for b in range(TOPB_DEV):
        source = top_source[b]
        lhs, rhs = [], []
        for c in range(8):
            child = gathered[source * 8 + c]
            lhs.append(stacked_groups(child[40:48]))
            rhs.append(four_times(child[:K]))
        lifted = jnp.dot(
            jnp.concatenate(lhs, axis=1).astype(bf16),
            jnp.concatenate(rhs, axis=0),
            preferred_element_type=f32,
        )
        product = jnp.dot(
            stacked_groups(top_tiles[b]).astype(bf16),
            four_times(unpermute(lifted)),
            preferred_element_type=f32,
        )
        target = top_target[b]
        top_sum[target] = top_sum[target] + product
    for t in range(NTOP):
        top_rows[t] = unpermute(top_sum[t])

    def one(d, carry):
        lhs, rhs = [], []
        for slot in (first, second):
            b = slot[d]
            lhs.append(stacked_groups(tiles[b]))
            rhs.append(four_times(gathered[sources[b], :K]))
        lhs.append(stacked_groups(gathered[d, 32:40]))
        rhs.append(four_times(top_rows[d // 8]))
        out[d] = jnp.dot(
            jnp.concatenate(lhs, axis=1).astype(bf16),
            jnp.concatenate(rhs, axis=0),
            preferred_element_type=f32,
        ).astype(bf16)
        return carry

    lax.fori_loop(0, NBASE, one, 0, unroll=8)


def pieces(values):
    high = values.astype(bf16).astype(f32)
    rest = values - high
    middle = rest.astype(bf16).astype(f32)
    low = (rest - middle).astype(bf16).astype(f32)
    return high, middle, low


def features(points, source):
    row = lax.broadcasted_iota(jnp.int32, (8, M), 0)
    padded = jnp.concatenate([points, jnp.zeros((5, M), f32)], axis=0)
    centred = jnp.where(row < 3, (padded - 0.5) * math.sqrt(near_scale_sq), 0.0)
    norm = jnp.sum(centred * centred, axis=0, keepdims=True)
    if source:
        norm = norm + delta_sq * near_scale_sq
    norm = jnp.broadcast_to(norm, (8, M))
    high, middle, low = pieces(centred)
    norms = pieces(norm)
    one = jnp.ones((8, M), f32)
    if source:
        groups = [high, middle, high, low, high, middle]
    else:
        groups = [-2 * high, -2 * high, -2 * middle, -2 * high, -2 * low, -2 * middle]
    done = []
    for i, part in enumerate(groups):
        if i < 3:
            third, fourth = (one, norms[i]) if source else (norms[i], one)
            part = jnp.where(row == 3, third, jnp.where(row == 4, fourth, part))
        done.append(part)
    return jnp.concatenate(done, axis=0)


def near_kernel(
    columns, xb, xo, xa, qb, qo, qa, out, pool, feats, targets, kernel_a, kernel_b, sems
):
    L = LEAVES_DEV
    copies = [
        pltpu.make_async_copy(part, pool.at[pl.ds(i * L, L)], sems.at[i])
        for i, part in enumerate((qb, qo, qa))
    ]
    for copy in copies:
        copy.start()
    for i, part in enumerate((xb, xo, xa)):

        def prepare(g, carry, i=i, part=part):
            points = part[:, pl.ds(pl.multiple_of(g * M, M), M)]
            feats[i * L + g] = features(points, True).astype(bf16)
            if i == 1:
                targets[g] = features(points, False).T.astype(bf16)
            return carry

        lax.fori_loop(0, L, prepare, 0, unroll=8)
    for copy in copies:
        copy.wait()

    def weigh(l, store):
        mine = targets[l]
        for j in range(0, NNEAR, 2):
            named = [columns[l * NNEAR + k] for k in range(j, min(j + 2, NNEAR))]
            theirs = jnp.concatenate([feats[g] for g in named], axis=1)
            squares = jnp.dot(mine, theirs, preferred_element_type=f32)
            store[:, pl.ds(j * M, len(named) * M)] = lax.rsqrt(squares).astype(bf16)

    def apply(l, store):
        named = jnp.concatenate([pool[columns[l * NNEAR + j]] for j in range(NNEAR)], axis=0)
        out[l] = jnp.dot(store[...], named, preferred_element_type=f32)

    weigh(0, kernel_a)

    def two(i, carry):
        weigh(2 * i + 1, kernel_b)
        apply(2 * i, kernel_a)
        weigh(jnp.minimum(2 * i + 2, L - 1), kernel_a)
        apply(2 * i + 1, kernel_b)
        return carry

    lax.fori_loop(0, L // 2, two, 0)


def down_kernel(parts, vt, near, out, field):
    @pl.when(pl.program_id(0) == 0)
    def _():
        field[...] = unpermute(jnp.sum(parts[...].astype(f32), axis=0))

    for c in range(8):
        far = lax.dot_general(
            vt[c], field[...], (((0,), (0,)), ((), ())), preferred_element_type=f32
        )
        out[c] = (near[c] + far).astype(bf16)


def per_device(
    coords,
    charges,
    near_leaves,
    leaf_basis,
    leaf_transfer,
    mid_transfer,
    base_transfer,
    base_coupling,
    base_target,
    base_source,
    top_coupling,
    top_target,
    top_source,
):
    L = LEAVES_DEV
    size = lax.axis_size(LEAF)
    up = [(i, i + 1) for i in range(size - 1)]
    down = [(j, i) for i, j in up]
    q = charges.reshape(L, M, RHS)
    q_before = lax.ppermute(q, LEAF, up)
    q_after = lax.ppermute(q, LEAF, down)
    x_before = lax.ppermute(coords, LEAF, up)
    x_after = lax.ppermute(coords, LEAF, down)

    basis = leaf_basis.reshape(L, 8, 4, M).transpose(0, 2, 1, 3).reshape(L, K, M)
    lift = base_transfer.reshape(8, 128)
    lift_t = base_transfer.reshape(K, 8, 4).transpose(1, 2, 0).reshape(8, 128)
    message, vt = pl.pallas_call(
        up_kernel,
        out_shape=(
            jax.ShapeDtypeStruct((NBASE, MSG, RHS), bf16),
            jax.ShapeDtypeStruct((L, K, M), bf16),
        ),
        in_specs=[in_vmem()] * 6,
        out_specs=(in_vmem(), in_vmem()),
        name="up",
        cost_estimate=pl.CostEstimate(flops=2 * 10**9, bytes_accessed=5 * 10**6, transcendentals=0),
    )(
        q,
        basis,
        leaf_transfer.reshape(L, 8, 128),
        mid_transfer.reshape(MIDS_DEV, 8, 128),
        lift,
        lift_t,
    )
    gathered = lax.all_to_all(message, LEAF, 0, 0, tiled=True)

    names = jnp.arange(NBASE, dtype=jnp.int32)[:, None]
    places = jnp.arange(BLK_DEV, dtype=jnp.int32)[None, :]
    here = names == base_target[:, 0][None, :]
    first = jnp.min(jnp.where(here, places, BLK_DEV), axis=1)
    last = jnp.max(jnp.where(here, places, -1), axis=1)
    second = jnp.where(last > first, last, BLK_DEV)
    spare = BLK_PAD - BLK_DEV
    tiles = jnp.pad(base_coupling, ((0, spare), (0, 0))).reshape(BLK_PAD, 8, 128)
    sources = jnp.pad(base_source, (0, spare))
    partial = pl.pallas_call(
        couple_kernel,
        out_shape=jax.ShapeDtypeStruct((NBASE, K, RHS), bf16),
        in_specs=[in_smem()] * 5 + [in_vmem()] * 3,
        out_specs=in_vmem(),
        scratch_shapes=[
            pltpu.VMEM((NTOP, K, RHS), f32),
            pltpu.VMEM((NTOP, K, RHS), bf16),
        ],
        name="couple",
        cost_estimate=pl.CostEstimate(flops=2 * 10**9, bytes_accessed=5 * 10**6, transcendentals=0),
    )(
        first,
        second,
        sources,
        top_target,
        top_source,
        gathered,
        tiles,
        top_coupling.reshape(TOPB_DEV, 8, 128),
    )
    parts = lax.all_to_all(partial, LEAF, 0, 0, tiled=True)

    near = pl.pallas_call(
        near_kernel,
        out_shape=jax.ShapeDtypeStruct((L, M, RHS), f32),
        in_specs=[in_smem()] + [in_vmem()] * 3 + [in_place()] * 3,
        out_specs=in_vmem(),
        scratch_shapes=[
            pltpu.VMEM((3 * L, M, RHS), bf16),
            pltpu.VMEM((3 * L, FEAT, M), bf16),
            pltpu.VMEM((L, M, FEAT), bf16),
            pltpu.VMEM((M, NNEAR * M), bf16),
            pltpu.VMEM((M, NNEAR * M), bf16),
            pltpu.SemaphoreType.DMA((3,)),
        ],
        name="near",
        cost_estimate=pl.CostEstimate(flops=4 * 10**10, bytes_accessed=10**7, transcendentals=3 * 10**7),
    )(near_leaves.reshape(-1), x_before, coords, x_after, q_before, q, q_after)

    potential = pl.pallas_call(
        down_kernel,
        grid=(8,),
        out_shape=jax.ShapeDtypeStruct((L, M, RHS), bf16),
        in_specs=[
            pl.BlockSpec((NBASE, K, RHS), lambda i: (0, 0, 0)),
            pl.BlockSpec((8, K, M), lambda i: (i, 0, 0)),
            pl.BlockSpec((8, M, RHS), lambda i: (i, 0, 0)),
        ],
        out_specs=pl.BlockSpec((8, M, RHS), lambda i: (i, 0, 0)),
        scratch_shapes=[pltpu.VMEM((K, RHS), bf16)],
        name="down",
    )(parts, vt, near)
    return potential.reshape(L * M, RHS)


def solution(mesh):
    split = Mesh(mesh.devices.reshape(4, 4, 4, 2), LEAF)
    by_leaf = P(LEAF, None)
    in_specs = (P(None, LEAF),) + (by_leaf,) * 8 + (P(LEAF), by_leaf, P(LEAF), P(LEAF))
    return jax.shard_map(
        per_device, mesh=split, in_specs=in_specs, out_specs=by_leaf, check_vma=False
    )
```

```python
import math

import jax
import jax.numpy as jnp
from jax import lax
from jax.experimental import pallas as pl
from jax.experimental.pallas import tpu as pltpu
from jax.sharding import Mesh
from jax.sharding import PartitionSpec as P

K = 32
RHS = 128
M = 128
NNEAR = 27
LEAVES_DEV = 64
MIDS_DEV = 8
NBASE = 128
CHIPS = 64
NTOP = 16
BLK_DEV = 189
BLK_PAD = 192
TOPB_DEV = 8
FEAT = 48
MSG = 48
LEAF = ("leaf_0", "leaf_1", "leaf_2", "leaf_3")
delta_sq = 0.0025
near_scale_sq = float(NNEAR * M)

f32 = jnp.float32
bf16 = jnp.bfloat16


def in_vmem():
    return pl.BlockSpec(memory_space=pltpu.VMEM)


def in_smem():
    return pl.BlockSpec(memory_space=pltpu.SMEM)


def in_place():
    return pl.BlockSpec(memory_space=pl.ANY)


def stacked_groups(tile):
    tile = tile.astype(f32)
    group = lax.broadcasted_iota(jnp.int32, tile.shape, 1) // K
    return jnp.concatenate([jnp.where(group == g, tile, 0.0) for g in range(4)], axis=0)


def rolled_groups(tile):
    tile = tile.astype(f32)
    lane = lax.broadcasted_iota(jnp.int32, tile.shape, 1)
    parts = [tile] + [pltpu.roll(tile, 128 - K * g, 1) for g in range(1, 4)]
    return jnp.concatenate([jnp.where(lane < K, part, 0.0) for part in parts], axis=0)


def unpermute(rows):
    to = lax.broadcasted_iota(jnp.int32, (K, K), 0)
    at = lax.broadcasted_iota(jnp.int32, (K, K), 1)
    order = jnp.where(to == 4 * (at % 8) + at // 8, 1.0, 0.0).astype(bf16)
    return jnp.dot(order, rows.astype(bf16), preferred_element_type=f32).astype(bf16)


def four_times(rows):
    return jnp.concatenate([rows] * 4, axis=0)


def up_kernel(q, basis, leaf_rows, mid_rows, lift_rows, message, v_rows, basis_s, leaf_s, mid_s, lift_s):
    for i in range(8):
        piece = pl.ds(i * 128, 128)
        mid_s[pl.ds(i, MIDS_DEV, stride=8), :] = mid_rows[:, piece].astype(f32)
        lift_s[pl.ds(i, 1), :] = lift_rows[:, piece].astype(f32)
    lift = lift_s[pl.ds(0, 8), :]
    straight = unpermute(rolled_groups(lift)).astype(f32)
    turned = jnp.concatenate([straight, jnp.zeros((96, 128), f32)], axis=0).T
    lift_t = turned[:8]
    for g in range(1, 4):
        lift_t = lift_t + pltpu.roll(turned[8 * g : 8 * g + 8], K * g, 1)

    coeffs = jnp.zeros((K, RHS), f32)
    for m in range(MIDS_DEV):
        own = pl.ds(8 * m, 8)
        for i in range(8):
            leaf_s[pl.ds(64 * m + i, 8, stride=8), :] = leaf_rows[own, pl.ds(i * 128, 128)].astype(f32)
        for k in range(K):
            at = 256 * m + 8 * (k % 4) + k // 4
            basis_s[pl.ds(at, 8, stride=K), :] = basis[own, pl.ds(k * M, M)].astype(f32)
        mid = four_times(unpermute(rolled_groups(mid_s[pl.ds(8 * m, 8), :])))
        lhs = [stacked_groups(leaf_s[pl.ds(64 * m + 8 * c, 8), :]) for c in range(8)]
        lhs = jnp.concatenate(lhs, axis=0).astype(bf16)
        through = jnp.dot(lhs, mid, preferred_element_type=f32)
        rows = []
        for c in range(8):
            back = through[K * c : K * (c + 1)].T[:K].astype(bf16)
            own_basis = basis_s[pl.ds(256 * m + K * c, K), :].astype(bf16)
            rows.append(jnp.dot(back, own_basis, preferred_element_type=f32))
        for h in range(2):
            four = jnp.concatenate(rows[4 * h : 4 * h + 4], axis=0)
            v_rows[2 * m + h] = four.T.astype(bf16)
        across = jnp.concatenate([row.astype(bf16) for row in rows], axis=1)
        four_k = q[own].reshape(8 * M, RHS)
        coeffs = coeffs + jnp.dot(across, four_k, preferred_element_type=f32)
    whole = jnp.concatenate([coeffs, lift, lift_t], axis=0).astype(bf16)

    def put(d, carry):
        message[d] = whole
        return carry

    lax.fori_loop(0, CHIPS, put, 0, unroll=8)


def couple_kernel(
    core, first, second, sources, top_target, top_source, mine, other, tiles, top_tiles, out,
    gathered, top_sum, top_rows, sems,
):
    me = core[0]
    copies = [
        pltpu.make_async_copy(mine, gathered.at[pl.ds(me * CHIPS, CHIPS)], sems.at[0]),
        pltpu.make_async_copy(other, gathered.at[pl.ds((1 - me) * CHIPS, CHIPS)], sems.at[1]),
    ]
    for copy in copies:
        copy.start()
    for copy in copies:
        copy.wait()

    top_sum[...] = jnp.zeros((NTOP, K, RHS), f32)
    lifted = []
    for b in range(TOPB_DEV):
        source = top_source[b]
        lhs, rhs = [], []
        for c in range(8):
            child = gathered[(c % 2) * CHIPS + source * 4 + c // 2]
            lhs.append(stacked_groups(child[40:48]))
            rhs.append(four_times(child[:K]))
        lifted.append(
            jnp.dot(
                jnp.concatenate(lhs, axis=1).astype(bf16),
                jnp.concatenate(rhs, axis=0),
                preferred_element_type=f32,
            ).astype(bf16)
        )
    products = [
        jnp.dot(
            stacked_groups(top_tiles[b]).astype(bf16),
            four_times(lifted[b]),
            preferred_element_type=f32,
        )
        for b in range(TOPB_DEV)
    ]
    for b in range(TOPB_DEV):
        target = top_target[b]
        top_sum[target] = top_sum[target] + products[b]
    every = jnp.concatenate([top_sum[t] for t in range(NTOP)], axis=1)
    every = unpermute(every)
    for t in range(NTOP):
        top_rows[t] = every[:, t * RHS : (t + 1) * RHS]

    def one(d, carry):
        lhs, rhs = [], []
        for slot in (first, second):
            b = slot[d]
            s = sources[b]
            lhs.append(stacked_groups(tiles[b]))
            rhs.append(four_times(gathered[(s % 2) * CHIPS + s // 2, :K]))
        lhs.append(stacked_groups(gathered[(d % 2) * CHIPS + d // 2, 32:40]))
        rhs.append(four_times(top_rows[d // 8]))
        out[d] = jnp.dot(
            jnp.concatenate(lhs, axis=1).astype(bf16),
            jnp.concatenate(rhs, axis=0),
            preferred_element_type=f32,
        ).astype(bf16)
        return carry

    lax.fori_loop(0, NBASE, one, 0, unroll=16)


def pieces(values):
    high = values.astype(bf16).astype(f32)
    rest = values - high
    middle = rest.astype(bf16).astype(f32)
    low = (rest - middle).astype(bf16).astype(f32)
    return high, middle, low


def features(points, source):
    row = lax.broadcasted_iota(jnp.int32, (8, M), 0)
    padded = jnp.concatenate([points, jnp.zeros((5, M), f32)], axis=0)
    centred = jnp.where(row < 3, (padded - 0.5) * math.sqrt(near_scale_sq), 0.0)
    norm = jnp.sum(centred * centred, axis=0, keepdims=True)
    if source:
        norm = norm + delta_sq * near_scale_sq
    norm = jnp.broadcast_to(norm, (8, M))
    high, middle, low = pieces(centred)
    norms = pieces(norm)
    one = jnp.ones((8, M), f32)
    if source:
        groups = [high, middle, high, low, high, middle]
    else:
        groups = [-2 * high, -2 * high, -2 * middle, -2 * high, -2 * low, -2 * middle]
    done = []
    for i, part in enumerate(groups):
        if i < 3:
            third, fourth = (one, norms[i]) if source else (norms[i], one)
            part = jnp.where(row == 3, third, jnp.where(row == 4, fourth, part))
        done.append(part)
    return jnp.concatenate(done, axis=0)


def near_kernel(
    columns, xb, xo, xa, qb, qo, qa, out, pool, feats, targets, kernel_a, kernel_b, sems
):
    L = LEAVES_DEV
    copies = [
        pltpu.make_async_copy(part, pool.at[pl.ds(i * L, L)], sems.at[i])
        for i, part in enumerate((qb, qo, qa))
    ]
    for copy in copies:
        copy.start()
    for i, part in enumerate((xb, xo, xa)):

        def prepare(g, carry, i=i, part=part):
            points = part[:, pl.ds(pl.multiple_of(g * M, M), M)]
            feats[i * L + g] = features(points, True).astype(bf16)
            if i == 1:
                targets[g] = features(points, False).T.astype(bf16)
            return carry

        lax.fori_loop(0, L, prepare, 0, unroll=8)
    for copy in copies:
        copy.wait()

    def weigh(l, store):
        mine = targets[l]
        for j in range(0, NNEAR, 2):
            named = [columns[l * NNEAR + k] for k in range(j, min(j + 2, NNEAR))]
            theirs = jnp.concatenate([feats[g] for g in named], axis=1)
            squares = jnp.dot(mine, theirs, preferred_element_type=f32)
            store[:, pl.ds(j * M, len(named) * M)] = lax.rsqrt(squares).astype(bf16)

    def apply(l, store):
        named = jnp.concatenate([pool[columns[l * NNEAR + j]] for j in range(NNEAR)], axis=0)
        out[l] = jnp.dot(store[...], named, preferred_element_type=f32)

    weigh(0, kernel_a)

    def two(i, carry):
        weigh(2 * i + 1, kernel_b)
        apply(2 * i, kernel_a)
        weigh(jnp.minimum(2 * i + 2, L - 1), kernel_a)
        apply(2 * i + 1, kernel_b)
        return carry

    lax.fori_loop(0, L // 2, two, 0)


def down_kernel(parts, v_rows, near, out, parts_s, v_s, near_s, out_s, sems):
    steps = LEAVES_DEV // 8
    chunks = [pl.ds(8 * i, 8) for i in range(steps)]
    first = [
        pltpu.make_async_copy(parts, parts_s, sems.at[0]),
        pltpu.make_async_copy(v_rows, v_s, sems.at[1]),
    ]
    loads = [
        pltpu.make_async_copy(near.at[c], near_s.at[c], sems.at[2 + i]) for i, c in enumerate(chunks)
    ]
    for copy in first + loads:
        copy.start()
    to = lax.broadcasted_iota(jnp.int32, (K, NBASE * K), 0)
    at = lax.broadcasted_iota(jnp.int32, (K, NBASE * K), 1) % K
    order = jnp.where(to == 4 * (at % 8) + at // 8, 1.0, 0.0).astype(bf16)
    first[0].wait()
    field = jnp.dot(order, parts_s[...].reshape(NBASE * K, RHS), preferred_element_type=f32)
    zero = jnp.zeros((K, RHS), f32)
    spread = [
        jnp.concatenate([field if g == h else zero for h in range(4)], axis=0) for g in range(4)
    ]
    spread = jnp.concatenate(spread, axis=1).astype(bf16)
    first[1].wait()
    stores = []
    for i, chunk in enumerate(chunks):
        rows = v_s[pl.ds(2 * i, 2)].reshape(2 * M, 4 * K)
        far = jnp.dot(rows, spread, preferred_element_type=f32)
        loads[i].wait()
        for c in range(8):
            h, g = c // 4, c % 4
            part = far[h * M : (h + 1) * M, g * RHS : (g + 1) * RHS]
            out_s[8 * i + c] = (near_s[8 * i + c] + part).astype(bf16)
        stores.append(pltpu.make_async_copy(out_s.at[chunk], out.at[chunk], sems.at[10 + i]))
        stores[-1].start()
    for copy in stores:
        copy.wait()


def per_device(
    coords,
    charges,
    near_leaves,
    leaf_basis,
    leaf_transfer,
    mid_transfer,
    base_transfer,
    base_coupling,
    base_target,
    base_source,
    top_coupling,
    top_target,
    top_source,
):
    L = LEAVES_DEV
    size = lax.axis_size(LEAF)
    up = [(i, i + 1) for i in range(size - 1)]
    down = [(j, i) for i, j in up]
    q = charges.reshape(L, M, RHS)
    q_before = lax.ppermute(q, LEAF, up)
    q_after = lax.ppermute(q, LEAF, down)
    x_before = lax.ppermute(coords, LEAF, up)
    x_after = lax.ppermute(coords, LEAF, down)

    message, v_rows = pl.pallas_call(
        up_kernel,
        out_shape=(
            jax.ShapeDtypeStruct((CHIPS, MSG, RHS), bf16),
            jax.ShapeDtypeStruct((L // 4, M, 4 * K), bf16),
        ),
        in_specs=[in_vmem()] * 5,
        out_specs=(in_vmem(), in_vmem()),
        scratch_shapes=[
            pltpu.VMEM((L * K, M), f32),
            pltpu.VMEM((L * 8, 128), f32),
            pltpu.VMEM((MIDS_DEV * 8, 128), f32),
            pltpu.VMEM((8, 128), f32),
        ],
        name="up",
        cost_estimate=pl.CostEstimate(flops=2 * 10**9, bytes_accessed=5 * 10**6, transcendentals=0),
    )(q, leaf_basis, leaf_transfer, mid_transfer, base_transfer)
    mine = lax.all_to_all(message, LEAF[:3], 0, 0, tiled=True)
    other = lax.ppermute(mine, LEAF[3], [(0, 1), (1, 0)])

    names = jnp.arange(NBASE, dtype=jnp.int32)[:, None]
    places = jnp.arange(BLK_DEV, dtype=jnp.int32)[None, :]
    here = names == base_target[:, 0][None, :]
    first = jnp.min(jnp.where(here, places, BLK_DEV), axis=1)
    last = jnp.max(jnp.where(here, places, -1), axis=1)
    second = jnp.where(last > first, last, BLK_DEV)
    spare = BLK_PAD - BLK_DEV
    tiles = jnp.pad(base_coupling, ((0, spare), (0, 0))).reshape(BLK_PAD, 8, 128)
    sources = jnp.pad(base_source, (0, spare))
    partial = pl.pallas_call(
        couple_kernel,
        out_shape=jax.ShapeDtypeStruct((NBASE, K, RHS), bf16),
        in_specs=[in_smem()] * 6 + [in_place()] * 2 + [in_vmem()] * 2,
        out_specs=in_vmem(),
        scratch_shapes=[
            pltpu.VMEM((NBASE, MSG, RHS), bf16),
            pltpu.VMEM((NTOP, K, RHS), f32),
            pltpu.VMEM((NTOP, K, RHS), bf16),
            pltpu.SemaphoreType.DMA((2,)),
        ],
        name="couple",
        cost_estimate=pl.CostEstimate(flops=2 * 10**9, bytes_accessed=5 * 10**6, transcendentals=0),
    )(
        lax.axis_index(LEAF[3]).reshape(1).astype(jnp.int32),
        first,
        second,
        sources,
        top_target,
        top_source,
        mine,
        other,
        tiles,
        top_coupling.reshape(TOPB_DEV, 8, 128),
    )
    parts = lax.all_to_all(partial, LEAF, 0, 0, tiled=True)

    near = pl.pallas_call(
        near_kernel,
        out_shape=jax.ShapeDtypeStruct((L, M, RHS), f32),
        in_specs=[in_smem()] + [in_vmem()] * 3 + [in_place()] * 3,
        out_specs=in_vmem(),
        scratch_shapes=[
            pltpu.VMEM((3 * L, M, RHS), bf16),
            pltpu.VMEM((3 * L, FEAT, M), bf16),
            pltpu.VMEM((L, M, FEAT), bf16),
            pltpu.VMEM((M, NNEAR * M), bf16),
            pltpu.VMEM((M, NNEAR * M), bf16),
            pltpu.SemaphoreType.DMA((3,)),
        ],
        name="near",
        cost_estimate=pl.CostEstimate(flops=4 * 10**10, bytes_accessed=10**7, transcendentals=3 * 10**7),
    )(near_leaves.reshape(-1), x_before, coords, x_after, q_before, q, q_after)

    potential = pl.pallas_call(
        down_kernel,
        out_shape=jax.ShapeDtypeStruct((L, M, RHS), bf16),
        in_specs=[in_place()] * 3,
        out_specs=in_place(),
        scratch_shapes=[
            pltpu.VMEM((NBASE, K, RHS), bf16),
            pltpu.VMEM((L // 4, M, 4 * K), bf16),
            pltpu.VMEM((L, M, RHS), f32),
            pltpu.VMEM((L, M, RHS), bf16),
            pltpu.SemaphoreType.DMA((18,)),
        ],
        name="down",
        cost_estimate=pl.CostEstimate(flops=10**9, bytes_accessed=10**7, transcendentals=0),
    )(parts, v_rows, near)
    return potential.reshape(L * M, RHS)


def solution(mesh):
    split = Mesh(mesh.devices.reshape(4, 4, 4, 2), LEAF)
    by_leaf = P(LEAF, None)
    in_specs = (P(None, LEAF),) + (by_leaf,) * 8 + (P(LEAF), by_leaf, P(LEAF), P(LEAF))
    return jax.shard_map(
        per_device, mesh=split, in_specs=in_specs, out_specs=by_leaf, check_vma=False
    )
```

```python
import math

import jax
import jax.numpy as jnp
from jax import lax
from jax.experimental import pallas as pl
from jax.experimental.pallas import tpu as pltpu
from jax.sharding import Mesh
from jax.sharding import PartitionSpec as P

K = 32
RHS = 128
M = 128
NNEAR = 27
LEAVES_DEV = 64
MIDS_DEV = 8
NBASE = 128
CHIPS = 64
NTOP = 16
BLK_DEV = 189
BLK_PAD = 192
TOPB_DEV = 8
FEAT = 48
POINTS = 8192
TAIL = 576
MSG = 48
LEAF = ("leaf_0", "leaf_1", "leaf_2", "leaf_3")
delta_sq = 0.0025
near_scale_sq = float(NNEAR * M)

f32 = jnp.float32
bf16 = jnp.bfloat16


def in_vmem():
    return pl.BlockSpec(memory_space=pltpu.VMEM)


def in_smem():
    return pl.BlockSpec(memory_space=pltpu.SMEM)


def in_place():
    return pl.BlockSpec(memory_space=pl.ANY)


def stacked_groups(tile):
    tile = tile.astype(f32)
    group = lax.broadcasted_iota(jnp.int32, tile.shape, 1) // K
    return jnp.concatenate([jnp.where(group == g, tile, 0.0) for g in range(4)], axis=0)


def rolled_groups(tile):
    tile = tile.astype(f32)
    lane = lax.broadcasted_iota(jnp.int32, tile.shape, 1)
    parts = [tile] + [pltpu.roll(tile, 128 - K * g, 1) for g in range(1, 4)]
    return jnp.concatenate([jnp.where(lane < K, part, 0.0) for part in parts], axis=0)


def unpermute(rows):
    to = lax.broadcasted_iota(jnp.int32, (K, K), 0)
    at = lax.broadcasted_iota(jnp.int32, (K, K), 1)
    order = jnp.where(to == 4 * (at % 8) + at // 8, 1.0, 0.0).astype(bf16)
    return jnp.dot(order, rows.astype(bf16), preferred_element_type=f32).astype(bf16)


def four_times(rows):
    return jnp.concatenate([rows] * 4, axis=0)


def up_kernel(
    q, coords, basis, leaf_rows, mid_rows, lift_rows, message, v_rows, halo,
    basis_s, leaf_s, mid_s, lift_s, points_s, tail_s, sems,
):
    bulk = pltpu.make_async_copy(q, halo.at[pl.ds(0, POINTS)], sems.at[0])
    bulk.start()

    def spread(g, carry):
        row = coords[:, pl.ds(pl.multiple_of(g * M, M), M)]
        points_s[pl.ds(g, 3, stride=LEAVES_DEV), :] = row
        return carry

    lax.fori_loop(0, LEAVES_DEV, spread, 0, unroll=8)
    for i, piece in enumerate(pieces(points_s[...])):
        tail_s[pl.ds(i * 3 * LEAVES_DEV, 3 * LEAVES_DEV), :] = piece.astype(bf16)
    tail = pltpu.make_async_copy(tail_s, halo.at[pl.ds(POINTS, TAIL)], sems.at[1])
    tail.start()

    for i in range(8):
        piece = pl.ds(i * 128, 128)
        mid_s[pl.ds(i, MIDS_DEV, stride=8), :] = mid_rows[:, piece].astype(f32)
        lift_s[pl.ds(i, 1), :] = lift_rows[:, piece].astype(f32)
    lift = lift_s[pl.ds(0, 8), :]
    straight = unpermute(rolled_groups(lift)).astype(f32)
    turned = jnp.concatenate([straight, jnp.zeros((96, 128), f32)], axis=0).T
    lift_t = turned[:8]
    for g in range(1, 4):
        lift_t = lift_t + pltpu.roll(turned[8 * g : 8 * g + 8], K * g, 1)

    coeffs = jnp.zeros((K, RHS), f32)
    for m in range(MIDS_DEV):
        own = pl.ds(8 * m, 8)
        for i in range(8):
            leaf_s[pl.ds(64 * m + i, 8, stride=8), :] = leaf_rows[own, pl.ds(i * 128, 128)].astype(f32)
        for k in range(K):
            at = 256 * m + 8 * (k % 4) + k // 4
            basis_s[pl.ds(at, 8, stride=K), :] = basis[own, pl.ds(k * M, M)].astype(f32)
        mid = four_times(unpermute(rolled_groups(mid_s[pl.ds(8 * m, 8), :])))
        lhs = [stacked_groups(leaf_s[pl.ds(64 * m + 8 * c, 8), :]) for c in range(8)]
        lhs = jnp.concatenate(lhs, axis=0).astype(bf16)
        through = jnp.dot(lhs, mid, preferred_element_type=f32)
        rows = []
        for c in range(8):
            back = through[K * c : K * (c + 1)].T[:K].astype(bf16)
            own_basis = basis_s[pl.ds(256 * m + K * c, K), :].astype(bf16)
            rows.append(jnp.dot(back, own_basis, preferred_element_type=f32))
        for h in range(2):
            four = jnp.concatenate(rows[4 * h : 4 * h + 4], axis=0)
            v_rows[2 * m + h] = four.T.astype(bf16)
        across = jnp.concatenate([row.astype(bf16) for row in rows], axis=1)
        coeffs = coeffs + jnp.dot(
            across, q[pl.ds(8 * m * M, 8 * M)], preferred_element_type=f32
        )
    whole = jnp.concatenate([coeffs, lift, lift_t], axis=0).astype(bf16)

    def put(d, carry):
        message[d] = whole
        return carry

    lax.fori_loop(0, CHIPS, put, 0, unroll=8)
    bulk.wait()
    tail.wait()


def couple_kernel(
    core, table, sources, top_target, top_source, mine, other, tiles, top_tiles, out,
    gathered, top_sum, top_rows, sems,
):
    me = core[0]
    copies = [
        pltpu.make_async_copy(mine, gathered.at[pl.ds(me * CHIPS, CHIPS)], sems.at[0]),
        pltpu.make_async_copy(other, gathered.at[pl.ds((1 - me) * CHIPS, CHIPS)], sems.at[1]),
    ]
    for copy in copies:
        copy.start()
    for copy in copies:
        copy.wait()
    top_sum[...] = jnp.zeros((NTOP, K, RHS), f32)
    lifted = []
    for b in range(TOPB_DEV):
        source = top_source[b]
        lhs, rhs = [], []
        for c in range(8):
            child = gathered[(c % 2) * CHIPS + source * 4 + c // 2]
            lhs.append(stacked_groups(child[40:48]))
            rhs.append(four_times(child[:K]))
        lifted.append(
            jnp.dot(
                jnp.concatenate(lhs, axis=1).astype(bf16),
                jnp.concatenate(rhs, axis=0),
                preferred_element_type=f32,
            ).astype(bf16)
        )
    products = [
        jnp.dot(
            stacked_groups(top_tiles[b]).astype(bf16),
            four_times(lifted[b]),
            preferred_element_type=f32,
        )
        for b in range(TOPB_DEV)
    ]
    for b in range(TOPB_DEV):
        target = top_target[b]
        top_sum[target] = top_sum[target] + products[b]
    every = jnp.concatenate([top_sum[t] for t in range(NTOP)], axis=1)
    every = unpermute(every)
    for t in range(NTOP):
        top_rows[t] = every[:, t * RHS : (t + 1) * RHS]

    def one(d, carry):
        lhs, rhs = [], []
        for row in (0, 1):
            b = table[row, d]
            s = sources[b]
            lhs.append(stacked_groups(tiles[b]))
            rhs.append(four_times(gathered[(s % 2) * CHIPS + s // 2, :K]))
        lhs.append(stacked_groups(gathered[(d % 2) * CHIPS + d // 2, 32:40]))
        rhs.append(four_times(top_rows[d // 8]))
        out[d] = jnp.dot(
            jnp.concatenate(lhs, axis=1).astype(bf16),
            jnp.concatenate(rhs, axis=0),
            preferred_element_type=f32,
        ).astype(bf16)
        return carry

    lax.fori_loop(0, NBASE, one, 0, unroll=16)


def pieces(values):
    high = values.astype(bf16).astype(f32)
    rest = values - high
    middle = rest.astype(bf16).astype(f32)
    low = (rest - middle).astype(bf16).astype(f32)
    return high, middle, low


def features(points, source):
    row = lax.broadcasted_iota(jnp.int32, (8, M), 0)
    padded = jnp.concatenate([points, jnp.zeros((5, M), f32)], axis=0)
    centred = jnp.where(row < 3, (padded - 0.5) * math.sqrt(near_scale_sq), 0.0)
    norm = jnp.sum(centred * centred, axis=0, keepdims=True)
    if source:
        norm = norm + delta_sq * near_scale_sq
    norm = jnp.broadcast_to(norm, (8, M))
    high, middle, low = pieces(centred)
    norms = pieces(norm)
    one = jnp.ones((8, M), f32)
    if source:
        groups = [high, middle, high, low, high, middle]
    else:
        groups = [-2 * high, -2 * high, -2 * middle, -2 * high, -2 * low, -2 * middle]
    done = []
    for i, part in enumerate(groups):
        if i < 3:
            third, fourth = (one, norms[i]) if source else (norms[i], one)
            part = jnp.where(row == 3, third, jnp.where(row == 4, fourth, part))
        done.append(part)
    return jnp.concatenate(done, axis=0)


def early_kernel(base_target, coords, table, feats, aims):
    targets = base_target[...]
    block = lax.broadcasted_iota(jnp.int32, (BLK_DEV, NBASE), 0)
    here = targets == lax.broadcasted_iota(jnp.int32, (BLK_DEV, NBASE), 1)
    first = jnp.min(jnp.where(here, block, BLK_DEV), axis=0, keepdims=True)
    last = jnp.max(jnp.where(here, block, -1), axis=0, keepdims=True)
    table[...] = jnp.zeros((8, NBASE), jnp.int32)
    table[0:1] = first
    table[1:2] = jnp.where(last > first, last, BLK_DEV)

    def prepare(g, carry):
        points = coords[:, pl.ds(pl.multiple_of(g * M, M), M)]
        feats[g] = features(points, True).astype(bf16)
        aims[g] = features(points, False).T.astype(bf16)
        return carry

    lax.fori_loop(0, LEAVES_DEV, prepare, 0, unroll=8)


def near_kernel(
    columns, own_feats, own_aims, before, own, after, out,
    pool, feats, aims, tails, points_s, kernel_a, kernel_b, sems,
):
    L = LEAVES_DEV
    tail_copies = [
        pltpu.make_async_copy(part.at[pl.ds(POINTS, TAIL)], tails.at[i], sems.at[i])
        for i, part in enumerate((before, after))
    ]
    copies = [
        pltpu.make_async_copy(own_aims, aims, sems.at[2]),
        pltpu.make_async_copy(own_feats, feats.at[pl.ds(L, L)], sems.at[3]),
    ]
    copies += [
        pltpu.make_async_copy(
            part.at[pl.ds(0, POINTS)], pool.at[pl.ds(i * POINTS, POINTS)], sems.at[4 + i]
        )
        for i, part in enumerate((before, own, after))
    ]
    for copy in tail_copies + copies:
        copy.start()
    for i in range(2):
        tail_copies[i].wait()
        part = [tails[i, pl.ds(p * 3 * L, 3 * L)].astype(f32) for p in range(3)]
        points_s[i] = part[0] + part[1] + part[2]

        def prepare(g, carry, i=i):
            points = points_s[i, pl.ds(g, 3, stride=L), :]
            feats[2 * i * L + g] = features(points, True).astype(bf16)
            return carry

        lax.fori_loop(0, L, prepare, 0, unroll=8)
    for copy in copies:
        copy.wait()

    def weigh(l, store):
        mine = aims[l]
        for j in range(0, NNEAR, 2):
            named = [columns[l * NNEAR + k] for k in range(j, min(j + 2, NNEAR))]
            theirs = jnp.concatenate([feats[g] for g in named], axis=1)
            squares = jnp.dot(mine, theirs, preferred_element_type=f32)
            store[:, pl.ds(j * M, len(named) * M)] = lax.rsqrt(squares).astype(bf16)

    def apply(l, store):
        starts = [pl.multiple_of(columns[l * NNEAR + j] * M, M) for j in range(NNEAR)]
        named = jnp.concatenate([pool[pl.ds(start, M)] for start in starts], axis=0)
        out[l] = jnp.dot(store[...], named, preferred_element_type=f32)

    weigh(0, kernel_a)

    def two(i, carry):
        weigh(2 * i + 1, kernel_b)
        apply(2 * i, kernel_a)
        weigh(jnp.minimum(2 * i + 2, L - 1), kernel_a)
        apply(2 * i + 1, kernel_b)
        return carry

    lax.fori_loop(0, L // 2, two, 0)


def down_kernel(parts, v_rows, near, out, parts_s, v_s, near_s, out_s, sems):
    steps = LEAVES_DEV // 8
    chunks = [pl.ds(8 * i, 8) for i in range(steps)]
    first = [
        pltpu.make_async_copy(parts, parts_s, sems.at[0]),
        pltpu.make_async_copy(v_rows, v_s, sems.at[1]),
    ]
    loads = [
        pltpu.make_async_copy(near.at[c], near_s.at[c], sems.at[2 + i])
        for i, c in enumerate(chunks)
    ]
    for copy in first + loads:
        copy.start()
    to = lax.broadcasted_iota(jnp.int32, (K, NBASE * K), 0)
    at = lax.broadcasted_iota(jnp.int32, (K, NBASE * K), 1) % K
    order = jnp.where(to == 4 * (at % 8) + at // 8, 1.0, 0.0).astype(bf16)
    first[0].wait()
    field = jnp.dot(order, parts_s[...].reshape(NBASE * K, RHS), preferred_element_type=f32)
    zero = jnp.zeros((K, RHS), f32)
    spread = [
        jnp.concatenate([field if g == h else zero for h in range(4)], axis=0) for g in range(4)
    ]
    spread = jnp.concatenate(spread, axis=1).astype(bf16)
    first[1].wait()
    stores = []
    for i, chunk in enumerate(chunks):
        rows = v_s[pl.ds(2 * i, 2)].reshape(2 * M, 4 * K)
        far = jnp.dot(rows, spread, preferred_element_type=f32)
        loads[i].wait()
        for c in range(8):
            h, g = c // 4, c % 4
            part = far[h * M : (h + 1) * M, g * RHS : (g + 1) * RHS]
            out_s[8 * i + c] = (near_s[8 * i + c] + part).astype(bf16)
        stores.append(pltpu.make_async_copy(out_s.at[chunk], out.at[chunk], sems.at[10 + i]))
        stores[-1].start()
    for copy in stores:
        copy.wait()


def all_steps(
    coords, charges, near_leaves, leaf_basis, leaf_transfer, mid_transfer, base_transfer,
    base_coupling, base_target, base_source, top_coupling, top_target, top_source,
):
    L = LEAVES_DEV
    size = lax.axis_size(LEAF)
    up = [(i, i + 1) for i in range(size - 1)]
    down = [(j, i) for i, j in up]
    message, v_rows, halo = pl.pallas_call(
        up_kernel,
        out_shape=(
            jax.ShapeDtypeStruct((CHIPS, MSG, RHS), bf16),
            jax.ShapeDtypeStruct((L // 4, M, 4 * K), bf16),
            jax.ShapeDtypeStruct((POINTS + TAIL, RHS), bf16),
        ),
        in_specs=[in_vmem()] * 6,
        out_specs=(in_vmem(), in_vmem(), in_place()),
        scratch_shapes=[
            pltpu.VMEM((L * K, M), f32),
            pltpu.VMEM((L * 8, 128), f32),
            pltpu.VMEM((MIDS_DEV * 8, 128), f32),
            pltpu.VMEM((8, 128), f32),
            pltpu.VMEM((3 * L, M), f32),
            pltpu.VMEM((TAIL, M), bf16),
            pltpu.SemaphoreType.DMA((2,)),
        ],
        name="up",
        cost_estimate=pl.CostEstimate(flops=2 * 10**9, bytes_accessed=5 * 10**6, transcendentals=0),
    )(charges, coords, leaf_basis, leaf_transfer, mid_transfer, base_transfer)
    mine = lax.all_to_all(message, LEAF[:3], 0, 0, tiled=True)
    other = lax.ppermute(mine, LEAF[3], [(0, 1), (1, 0)])
    before = lax.ppermute(halo, LEAF, up)
    after = lax.ppermute(halo, LEAF, down)

    table, own_feats, own_aims = pl.pallas_call(
        early_kernel,
        out_shape=(
            jax.ShapeDtypeStruct((8, NBASE), jnp.int32),
            jax.ShapeDtypeStruct((L, FEAT, M), bf16),
            jax.ShapeDtypeStruct((L, M, FEAT), bf16),
        ),
        in_specs=[in_vmem()] * 2,
        out_specs=(in_vmem(),) * 3,
        name="early",
        cost_estimate=pl.CostEstimate(flops=10**9, bytes_accessed=10**6, transcendentals=0),
    )(base_target, coords)

    spare = BLK_PAD - BLK_DEV
    tiles = jnp.pad(base_coupling, ((0, spare), (0, 0))).reshape(BLK_PAD, 8, 128)
    sources = jnp.pad(base_source, (0, spare))
    partial = pl.pallas_call(
        couple_kernel,
        out_shape=jax.ShapeDtypeStruct((NBASE, K, RHS), bf16),
        in_specs=[in_smem()] * 5 + [in_place()] * 2 + [in_vmem()] * 2,
        out_specs=in_vmem(),
        scratch_shapes=[
            pltpu.VMEM((NBASE, MSG, RHS), bf16),
            pltpu.VMEM((NTOP, K, RHS), f32),
            pltpu.VMEM((NTOP, K, RHS), bf16),
            pltpu.SemaphoreType.DMA((2,)),
        ],
        name="couple",
        cost_estimate=pl.CostEstimate(flops=2 * 10**9, bytes_accessed=5 * 10**6, transcendentals=0),
    )(
        lax.axis_index(LEAF[3]).reshape(1).astype(jnp.int32),
        table,
        sources,
        top_target,
        top_source,
        mine,
        other,
        tiles,
        top_coupling.reshape(TOPB_DEV, 8, 128),
    )
    parts = lax.all_to_all(partial, LEAF, 0, 0, tiled=True)

    near = pl.pallas_call(
        near_kernel,
        out_shape=jax.ShapeDtypeStruct((L, M, RHS), f32),
        in_specs=[in_smem()] + [in_place()] * 5,
        out_specs=in_vmem(),
        scratch_shapes=[
            pltpu.VMEM((3 * POINTS, RHS), bf16),
            pltpu.VMEM((3 * L, FEAT, M), bf16),
            pltpu.VMEM((L, M, FEAT), bf16),
            pltpu.VMEM((2, TAIL, M), bf16),
            pltpu.VMEM((2, 3 * L, M), f32),
            pltpu.VMEM((M, NNEAR * M), bf16),
            pltpu.VMEM((M, NNEAR * M), bf16),
            pltpu.SemaphoreType.DMA((7,)),
        ],
        name="near",
        cost_estimate=pl.CostEstimate(
            flops=4 * 10**10, bytes_accessed=10**7, transcendentals=3 * 10**7
        ),
    )(near_leaves.reshape(-1), own_feats, own_aims, before, charges, after)

    potential = pl.pallas_call(
        down_kernel,
        out_shape=jax.ShapeDtypeStruct((L, M, RHS), bf16),
        in_specs=[in_place()] * 3,
        out_specs=in_place(),
        scratch_shapes=[
            pltpu.VMEM((NBASE, K, RHS), bf16),
            pltpu.VMEM((L // 4, M, 4 * K), bf16),
            pltpu.VMEM((L, M, RHS), f32),
            pltpu.VMEM((L, M, RHS), bf16),
            pltpu.SemaphoreType.DMA((18,)),
        ],
        name="down",
        cost_estimate=pl.CostEstimate(flops=10**9, bytes_accessed=10**7, transcendentals=0),
    )(parts, v_rows, near)
    return potential.reshape(L * M, RHS)


def solution(mesh):
    split = Mesh(mesh.devices.reshape(4, 4, 4, 2), LEAF)
    by_leaf = P(LEAF, None)
    in_specs = (P(None, LEAF),) + (by_leaf,) * 8 + (P(LEAF), by_leaf, P(LEAF), P(LEAF))
    return jax.shard_map(
        all_steps, mesh=split, in_specs=in_specs, out_specs=by_leaf, check_vma=False
    )
```

```python
import math

import jax
import jax.numpy as jnp
from jax import lax
from jax.experimental import pallas as pl
from jax.experimental.pallas import tpu as pltpu
from jax.sharding import Mesh
from jax.sharding import PartitionSpec as P

K = 32
RHS = 128
M = 128
NNEAR = 27
LEAVES_DEV = 64
MIDS_DEV = 8
NBASE = 128
CHIPS = 64
NTOP = 16
BLK_DEV = 189
BLK_PAD = 192
TOPB_DEV = 8
FEAT = 48
POINTS = 8192
TAIL = 576
MSG = 48
LEAF = ("leaf_0", "leaf_1", "leaf_2", "leaf_3")
delta_sq = 0.0025
near_scale_sq = float(NNEAR * M)

f32 = jnp.float32
bf16 = jnp.bfloat16


def in_vmem():
    return pl.BlockSpec(memory_space=pltpu.VMEM)


def in_smem():
    return pl.BlockSpec(memory_space=pltpu.SMEM)


def in_place():
    return pl.BlockSpec(memory_space=pl.ANY)


def stacked_groups(tile):
    tile = tile.astype(f32)
    group = lax.broadcasted_iota(jnp.int32, tile.shape, 1) // K
    return jnp.concatenate([jnp.where(group == g, tile, 0.0) for g in range(4)], axis=0)


def rolled_groups(tile):
    tile = tile.astype(f32)
    lane = lax.broadcasted_iota(jnp.int32, tile.shape, 1)
    parts = [tile] + [pltpu.roll(tile, 128 - K * g, 1) for g in range(1, 4)]
    return jnp.concatenate([jnp.where(lane < K, part, 0.0) for part in parts], axis=0)


def unpermute(rows):
    to = lax.broadcasted_iota(jnp.int32, (K, K), 0)
    at = lax.broadcasted_iota(jnp.int32, (K, K), 1)
    order = jnp.where(to == 4 * (at % 8) + at // 8, 1.0, 0.0).astype(bf16)
    return jnp.dot(order, rows.astype(bf16), preferred_element_type=f32).astype(bf16)


def four_times(rows):
    return jnp.concatenate([rows] * 4, axis=0)


def up_kernel(
    q, coords, basis, leaf_rows, mid_rows, lift_rows, message, v_rows, halo,
    basis_s, leaf_s, mid_s, lift_s, points_s, tail_s, sems,
):
    bulk = pltpu.make_async_copy(q, halo.at[pl.ds(0, POINTS)], sems.at[0])
    bulk.start()

    def spread(g, carry):
        row = coords[:, pl.ds(pl.multiple_of(g * M, M), M)]
        points_s[pl.ds(g, 3, stride=LEAVES_DEV), :] = row
        return carry

    lax.fori_loop(0, LEAVES_DEV, spread, 0, unroll=8)
    for i, piece in enumerate(pieces(points_s[...])):
        tail_s[pl.ds(i * 3 * LEAVES_DEV, 3 * LEAVES_DEV), :] = piece.astype(bf16)
    tail = pltpu.make_async_copy(tail_s, halo.at[pl.ds(POINTS, TAIL)], sems.at[1])
    tail.start()

    for i in range(8):
        piece = pl.ds(i * 128, 128)
        mid_s[pl.ds(i, MIDS_DEV, stride=8), :] = mid_rows[:, piece].astype(f32)
        lift_s[pl.ds(i, 1), :] = lift_rows[:, piece].astype(f32)
    lift = lift_s[pl.ds(0, 8), :]
    straight = unpermute(rolled_groups(lift)).astype(f32)
    turned = jnp.concatenate([straight, jnp.zeros((96, 128), f32)], axis=0).T
    lift_t = turned[:8]
    for g in range(1, 4):
        lift_t = lift_t + pltpu.roll(turned[8 * g : 8 * g + 8], K * g, 1)

    coeffs = jnp.zeros((K, RHS), f32)
    for m in range(MIDS_DEV):
        own = pl.ds(8 * m, 8)
        for i in range(8):
            leaf_s[pl.ds(64 * m + i, 8, stride=8), :] = leaf_rows[own, pl.ds(i * 128, 128)].astype(f32)
        for k in range(K):
            at = 256 * m + 8 * (k % 4) + k // 4
            basis_s[pl.ds(at, 8, stride=K), :] = basis[own, pl.ds(k * M, M)].astype(f32)
        mid = four_times(unpermute(rolled_groups(mid_s[pl.ds(8 * m, 8), :])))
        lhs = [stacked_groups(leaf_s[pl.ds(64 * m + 8 * c, 8), :]) for c in range(8)]
        lhs = jnp.concatenate(lhs, axis=0).astype(bf16)
        through = jnp.dot(lhs, mid, preferred_element_type=f32)
        rows = []
        for c in range(8):
            back = through[K * c : K * (c + 1)].T[:K].astype(bf16)
            own_basis = basis_s[pl.ds(256 * m + K * c, K), :].astype(bf16)
            rows.append(jnp.dot(back, own_basis, preferred_element_type=f32))
        for h in range(2):
            four = jnp.concatenate(rows[4 * h : 4 * h + 4], axis=0)
            v_rows[2 * m + h] = four.T.astype(bf16)
        across = jnp.concatenate([row.astype(bf16) for row in rows], axis=1)
        coeffs = coeffs + jnp.dot(
            across, q[pl.ds(8 * m * M, 8 * M)], preferred_element_type=f32
        )
    whole = jnp.concatenate([coeffs, lift, lift_t], axis=0).astype(bf16)

    def put(d, carry):
        message[d] = whole
        return carry

    lax.fori_loop(0, CHIPS, put, 0, unroll=8)
    bulk.wait()
    tail.wait()


def couple_kernel(
    core, table, sources, top_target, top_source, mine, other, tiles, top_tiles, out,
    gathered, top_sum, top_rows, sems,
):
    me = core[0]
    copies = [
        pltpu.make_async_copy(mine, gathered.at[pl.ds(me * CHIPS, CHIPS)], sems.at[0]),
        pltpu.make_async_copy(other, gathered.at[pl.ds((1 - me) * CHIPS, CHIPS)], sems.at[1]),
    ]
    for copy in copies:
        copy.start()
    for copy in copies:
        copy.wait()
    top_sum[...] = jnp.zeros((NTOP, K, RHS), f32)
    lifted = []
    for b in range(TOPB_DEV):
        source = top_source[b]
        lhs, rhs = [], []
        for c in range(8):
            child = gathered[(c % 2) * CHIPS + source * 4 + c // 2]
            lhs.append(stacked_groups(child[40:48]))
            rhs.append(four_times(child[:K]))
        lifted.append(
            jnp.dot(
                jnp.concatenate(lhs, axis=1).astype(bf16),
                jnp.concatenate(rhs, axis=0),
                preferred_element_type=f32,
            ).astype(bf16)
        )
    products = [
        jnp.dot(
            stacked_groups(top_tiles[b]).astype(bf16),
            four_times(lifted[b]),
            preferred_element_type=f32,
        )
        for b in range(TOPB_DEV)
    ]
    for b in range(TOPB_DEV):
        target = top_target[b]
        top_sum[target] = top_sum[target] + products[b]
    every = jnp.concatenate([top_sum[t] for t in range(NTOP)], axis=1)
    every = unpermute(every)
    for t in range(NTOP):
        top_rows[t] = every[:, t * RHS : (t + 1) * RHS]

    def one(d, carry):
        lhs, rhs = [], []
        for row in (0, 1):
            b = table[row, d]
            s = sources[b]
            lhs.append(stacked_groups(tiles[b]))
            rhs.append(four_times(gathered[(s % 2) * CHIPS + s // 2, :K]))
        lhs.append(stacked_groups(gathered[(d % 2) * CHIPS + d // 2, 32:40]))
        rhs.append(four_times(top_rows[d // 8]))
        out[d] = jnp.dot(
            jnp.concatenate(lhs, axis=1).astype(bf16),
            jnp.concatenate(rhs, axis=0),
            preferred_element_type=f32,
        ).astype(bf16)
        return carry

    lax.fori_loop(0, NBASE, one, 0, unroll=16)


def pieces(values):
    high = values.astype(bf16).astype(f32)
    rest = values - high
    middle = rest.astype(bf16).astype(f32)
    low = (rest - middle).astype(bf16).astype(f32)
    return high, middle, low


def features(points, source):
    row = lax.broadcasted_iota(jnp.int32, (8, M), 0)
    padded = jnp.concatenate([points, jnp.zeros((5, M), f32)], axis=0)
    centred = jnp.where(row < 3, (padded - 0.5) * math.sqrt(near_scale_sq), 0.0)
    norm = jnp.sum(centred * centred, axis=0, keepdims=True)
    if source:
        norm = norm + delta_sq * near_scale_sq
    norm = jnp.broadcast_to(norm, (8, M))
    high, middle, low = pieces(centred)
    norms = pieces(norm)
    one = jnp.ones((8, M), f32)
    if source:
        groups = [high, middle, high, low, high, middle]
    else:
        groups = [-2 * high, -2 * high, -2 * middle, -2 * high, -2 * low, -2 * middle]
    done = []
    for i, part in enumerate(groups):
        if i < 3:
            third, fourth = (one, norms[i]) if source else (norms[i], one)
            part = jnp.where(row == 3, third, jnp.where(row == 4, fourth, part))
        done.append(part)
    return jnp.concatenate(done, axis=0)


def early_kernel(base_target, coords, table, feats, aims):
    targets = base_target[...]
    block = lax.broadcasted_iota(jnp.int32, (BLK_DEV, NBASE), 0)
    here = targets == lax.broadcasted_iota(jnp.int32, (BLK_DEV, NBASE), 1)
    first = jnp.min(jnp.where(here, block, BLK_DEV), axis=0, keepdims=True)
    last = jnp.max(jnp.where(here, block, -1), axis=0, keepdims=True)
    table[...] = jnp.zeros((8, NBASE), jnp.int32)
    table[0:1] = first
    table[1:2] = jnp.where(last > first, last, BLK_DEV)

    def prepare(g, carry):
        points = coords[:, pl.ds(pl.multiple_of(g * M, M), M)]
        feats[g] = features(points, True).astype(bf16)
        aims[g] = features(points, False).astype(bf16)
        return carry

    lax.fori_loop(0, LEAVES_DEV, prepare, 0, unroll=8)


def near_kernel(
    columns, own_feats, own_aims, before, own, after, out,
    pool, feats, aims, tails, points_s, kernel_a, kernel_b, done, sems,
):
    L = LEAVES_DEV
    tail_copies = [
        pltpu.make_async_copy(part.at[pl.ds(POINTS, TAIL)], tails.at[i], sems.at[i])
        for i, part in enumerate((before, after))
    ]
    copies = [
        pltpu.make_async_copy(own_aims, aims, sems.at[2]),
        pltpu.make_async_copy(own_feats, feats.at[pl.ds(L, L)], sems.at[3]),
    ]
    copies += [
        pltpu.make_async_copy(
            part.at[pl.ds(0, POINTS)], pool.at[pl.ds(i * POINTS, POINTS)], sems.at[4 + i]
        )
        for i, part in enumerate((before, own, after))
    ]
    for copy in tail_copies + copies:
        copy.start()
    for i in range(2):
        tail_copies[i].wait()
        part = [tails[i, pl.ds(p * 3 * L, 3 * L)].astype(f32) for p in range(3)]
        points_s[i] = part[0] + part[1] + part[2]

        def prepare(g, carry, i=i):
            points = points_s[i, pl.ds(g, 3, stride=L), :]
            feats[2 * i * L + g] = features(points, True).astype(bf16)
            return carry

        lax.fori_loop(0, L, prepare, 0, unroll=8)
    for copy in copies:
        copy.wait()

    def weigh(l, store):
        mine = aims[l]
        for j in range(0, NNEAR, 2):
            named = [columns[l * NNEAR + k] for k in range(j, min(j + 2, NNEAR))]
            theirs = jnp.concatenate([feats[g] for g in named], axis=1)
            squares = lax.dot_general(
                mine, theirs, (((0,), (0,)), ((), ())), preferred_element_type=f32
            )
            store[:, pl.ds(j * M, len(named) * M)] = lax.rsqrt(squares).astype(bf16)

    def apply(l, store):
        starts = [pl.multiple_of(columns[l * NNEAR + j] * M, M) for j in range(NNEAR)]
        named = jnp.concatenate([pool[pl.ds(start, M)] for start in starts], axis=0)
        done[l] = jnp.dot(store[...], named, preferred_element_type=f32)

    weigh(0, kernel_a)

    def eight(i, carry):
        for l in range(0, 8, 2):
            weigh(8 * i + l + 1, kernel_b)
            apply(8 * i + l, kernel_a)
            weigh(jnp.minimum(8 * i + l + 2, L - 1), kernel_a)
            apply(8 * i + l + 1, kernel_b)
        part = pl.ds(8 * i, 8)
        pltpu.make_async_copy(done.at[part], out.at[part], sems.at[7]).start()
        return carry

    lax.fori_loop(0, L // 8, eight, 0)
    pltpu.make_async_copy(done, out, sems.at[7]).wait()


def down_kernel(parts, v_rows, near, out, parts_s, v_s, near_s, out_s, sems):
    steps = LEAVES_DEV // 8
    chunks = [pl.ds(8 * i, 8) for i in range(steps)]
    first = [
        pltpu.make_async_copy(parts, parts_s, sems.at[0]),
        pltpu.make_async_copy(v_rows, v_s, sems.at[1]),
    ]
    loads = [
        pltpu.make_async_copy(near.at[c], near_s.at[c], sems.at[2 + i])
        for i, c in enumerate(chunks)
    ]
    for copy in first + loads:
        copy.start()
    to = lax.broadcasted_iota(jnp.int32, (K, NBASE * K), 0)
    at = lax.broadcasted_iota(jnp.int32, (K, NBASE * K), 1) % K
    order = jnp.where(to == 4 * (at % 8) + at // 8, 1.0, 0.0).astype(bf16)
    first[0].wait()
    field = jnp.dot(order, parts_s[...].reshape(NBASE * K, RHS), preferred_element_type=f32)
    zero = jnp.zeros((K, RHS), f32)
    spread = [
        jnp.concatenate([field if g == h else zero for h in range(4)], axis=0) for g in range(4)
    ]
    spread = jnp.concatenate(spread, axis=1).astype(bf16)
    first[1].wait()
    stores = []
    for i, chunk in enumerate(chunks):
        rows = v_s[pl.ds(2 * i, 2)].reshape(2 * M, 4 * K)
        far = jnp.dot(rows, spread, preferred_element_type=f32)
        loads[i].wait()
        for c in range(8):
            h, g = c // 4, c % 4
            part = far[h * M : (h + 1) * M, g * RHS : (g + 1) * RHS]
            out_s[8 * i + c] = (near_s[8 * i + c] + part).astype(bf16)
        stores.append(pltpu.make_async_copy(out_s.at[chunk], out.at[chunk], sems.at[10 + i]))
        stores[-1].start()
    for copy in stores:
        copy.wait()


def all_steps(
    coords, charges, near_leaves, leaf_basis, leaf_transfer, mid_transfer, base_transfer,
    base_coupling, base_target, base_source, top_coupling, top_target, top_source,
):
    L = LEAVES_DEV
    size = lax.axis_size(LEAF)
    up = [(i, i + 1) for i in range(size - 1)]
    down = [(j, i) for i, j in up]
    message, v_rows, halo = pl.pallas_call(
        up_kernel,
        out_shape=(
            jax.ShapeDtypeStruct((CHIPS, MSG, RHS), bf16),
            jax.ShapeDtypeStruct((L // 4, M, 4 * K), bf16),
            jax.ShapeDtypeStruct((POINTS + TAIL, RHS), bf16),
        ),
        in_specs=[in_vmem()] * 6,
        out_specs=(in_vmem(), in_vmem(), in_place()),
        scratch_shapes=[
            pltpu.VMEM((L * K, M), f32),
            pltpu.VMEM((L * 8, 128), f32),
            pltpu.VMEM((MIDS_DEV * 8, 128), f32),
            pltpu.VMEM((8, 128), f32),
            pltpu.VMEM((3 * L, M), f32),
            pltpu.VMEM((TAIL, M), bf16),
            pltpu.SemaphoreType.DMA((2,)),
        ],
        name="up",
        cost_estimate=pl.CostEstimate(flops=2 * 10**9, bytes_accessed=5 * 10**6, transcendentals=0),
    )(charges, coords, leaf_basis, leaf_transfer, mid_transfer, base_transfer)
    mine = lax.all_to_all(message, LEAF[:3], 0, 0, tiled=True)
    other = lax.ppermute(mine, LEAF[3], [(0, 1), (1, 0)])
    before = lax.ppermute(halo, LEAF, up)
    after = lax.ppermute(halo, LEAF, down)

    table, own_feats, own_aims = pl.pallas_call(
        early_kernel,
        out_shape=(
            jax.ShapeDtypeStruct((8, NBASE), jnp.int32),
            jax.ShapeDtypeStruct((L, FEAT, M), bf16),
            jax.ShapeDtypeStruct((L, FEAT, M), bf16),
        ),
        in_specs=[in_vmem()] * 2,
        out_specs=(in_vmem(),) * 3,
        name="early",
        cost_estimate=pl.CostEstimate(flops=10**9, bytes_accessed=10**6, transcendentals=0),
    )(base_target, coords)

    spare = BLK_PAD - BLK_DEV
    tiles = jnp.pad(base_coupling, ((0, spare), (0, 0))).reshape(BLK_PAD, 8, 128)
    sources = jnp.pad(base_source, (0, spare))
    partial = pl.pallas_call(
        couple_kernel,
        out_shape=jax.ShapeDtypeStruct((NBASE, K, RHS), bf16),
        in_specs=[in_smem()] * 5 + [in_place()] * 2 + [in_vmem()] * 2,
        out_specs=in_vmem(),
        scratch_shapes=[
            pltpu.VMEM((NBASE, MSG, RHS), bf16),
            pltpu.VMEM((NTOP, K, RHS), f32),
            pltpu.VMEM((NTOP, K, RHS), bf16),
            pltpu.SemaphoreType.DMA((2,)),
        ],
        name="couple",
        cost_estimate=pl.CostEstimate(flops=2 * 10**9, bytes_accessed=5 * 10**6, transcendentals=0),
    )(
        lax.axis_index(LEAF[3]).reshape(1).astype(jnp.int32),
        table,
        sources,
        top_target,
        top_source,
        mine,
        other,
        tiles,
        top_coupling.reshape(TOPB_DEV, 8, 128),
    )
    parts = lax.all_to_all(partial, LEAF, 0, 0, tiled=True)

    near = pl.pallas_call(
        near_kernel,
        out_shape=jax.ShapeDtypeStruct((L, M, RHS), f32),
        in_specs=[in_smem()] + [in_place()] * 5,
        out_specs=in_place(),
        scratch_shapes=[
            pltpu.VMEM((3 * POINTS, RHS), bf16),
            pltpu.VMEM((3 * L, FEAT, M), bf16),
            pltpu.VMEM((L, FEAT, M), bf16),
            pltpu.VMEM((2, TAIL, M), bf16),
            pltpu.VMEM((2, 3 * L, M), f32),
            pltpu.VMEM((M, NNEAR * M), bf16),
            pltpu.VMEM((M, NNEAR * M), bf16),
            pltpu.VMEM((L, M, RHS), f32),
            pltpu.SemaphoreType.DMA((8,)),
        ],
        name="near",
        cost_estimate=pl.CostEstimate(
            flops=4 * 10**10, bytes_accessed=10**7, transcendentals=3 * 10**7
        ),
    )(near_leaves.reshape(-1), own_feats, own_aims, before, charges, after)

    potential = pl.pallas_call(
        down_kernel,
        out_shape=jax.ShapeDtypeStruct((L, M, RHS), bf16),
        in_specs=[in_place()] * 3,
        out_specs=in_place(),
        scratch_shapes=[
            pltpu.VMEM((NBASE, K, RHS), bf16),
            pltpu.VMEM((L // 4, M, 4 * K), bf16),
            pltpu.VMEM((L, M, RHS), f32),
            pltpu.VMEM((L, M, RHS), bf16),
            pltpu.SemaphoreType.DMA((18,)),
        ],
        name="down",
        cost_estimate=pl.CostEstimate(flops=10**9, bytes_accessed=10**7, transcendentals=0),
    )(parts, v_rows, near)
    return potential.reshape(L * M, RHS)


def solution(mesh):
    split = Mesh(mesh.devices.reshape(4, 4, 4, 2), LEAF)
    by_leaf = P(LEAF, None)
    in_specs = (P(None, LEAF),) + (by_leaf,) * 8 + (P(LEAF), by_leaf, P(LEAF), P(LEAF))
    return jax.shard_map(
        all_steps, mesh=split, in_specs=in_specs, out_specs=by_leaf, check_vma=False
    )
```

```python
import math

import jax
import jax.numpy as jnp
from jax import lax
from jax.experimental import pallas as pl
from jax.experimental.pallas import tpu as pltpu
from jax.sharding import Mesh
from jax.sharding import PartitionSpec as P

K = 32
RHS = 128
M = 128
NNEAR = 27
LEAVES_DEV = 64
MIDS_DEV = 8
NBASE = 128
CHIPS = 64
NTOP = 16
BLK_DEV = 189
TOPB_DEV = 8
FEAT = 48
OWN = 6
REST = NNEAR - OWN
UNITS = 8
SPARE = 40
POINTS = 8192
TAIL = 576
MSG = 48
LEAF = ("leaf_0", "leaf_1", "leaf_2", "leaf_3")
delta_sq = 0.0025
near_scale_sq = float(NNEAR * M)

f32 = jnp.float32
bf16 = jnp.bfloat16


def in_vmem():
    return pl.BlockSpec(memory_space=pltpu.VMEM)


def in_smem():
    return pl.BlockSpec(memory_space=pltpu.SMEM)


def in_place():
    return pl.BlockSpec(memory_space=pl.ANY)


def stacked_groups(tile):
    tile = tile.astype(f32)
    group = lax.broadcasted_iota(jnp.int32, tile.shape, 1) // K
    return jnp.concatenate([jnp.where(group == g, tile, 0.0) for g in range(4)], axis=0)


def rolled_groups(tile):
    tile = tile.astype(f32)
    lane = lax.broadcasted_iota(jnp.int32, tile.shape, 1)
    parts = [tile] + [pltpu.roll(tile, 128 - K * g, 1) for g in range(1, 4)]
    return jnp.concatenate([jnp.where(lane < K, part, 0.0) for part in parts], axis=0)


def unpermute(rows):
    to = lax.broadcasted_iota(jnp.int32, (K, K), 0)
    at = lax.broadcasted_iota(jnp.int32, (K, K), 1)
    order = jnp.where(to == 4 * (at % 8) + at // 8, 1.0, 0.0).astype(bf16)
    return jnp.dot(order, rows.astype(bf16), preferred_element_type=f32).astype(bf16)


def four_times(rows):
    return jnp.concatenate([rows] * 4, axis=0)


def up_kernel(
    q, coords, basis, leaf_rows, mid_rows, lift_rows, message, v_rows, halo,
    basis_s, leaf_s, mid_s, lift_s, points_s, tail_s, sems,
):
    bulk = pltpu.make_async_copy(q, halo.at[pl.ds(0, POINTS)], sems.at[0])
    bulk.start()

    def spread(g, carry):
        row = coords[:, pl.ds(pl.multiple_of(g * M, M), M)]
        points_s[pl.ds(g, 3, stride=LEAVES_DEV), :] = row
        return carry

    lax.fori_loop(0, LEAVES_DEV, spread, 0, unroll=8)
    for i, piece in enumerate(pieces(points_s[...])):
        tail_s[pl.ds(i * 3 * LEAVES_DEV, 3 * LEAVES_DEV), :] = piece.astype(bf16)
    tail = pltpu.make_async_copy(tail_s, halo.at[pl.ds(POINTS, TAIL)], sems.at[1])
    tail.start()

    for i in range(8):
        piece = pl.ds(i * 128, 128)
        mid_s[pl.ds(i, MIDS_DEV, stride=8), :] = mid_rows[:, piece].astype(f32)
        lift_s[pl.ds(i, 1), :] = lift_rows[:, piece].astype(f32)
    lift = lift_s[pl.ds(0, 8), :]
    straight = unpermute(rolled_groups(lift)).astype(f32)
    turned = jnp.concatenate([straight, jnp.zeros((96, 128), f32)], axis=0).T
    lift_t = turned[:8]
    for g in range(1, 4):
        lift_t = lift_t + pltpu.roll(turned[8 * g : 8 * g + 8], K * g, 1)

    coeffs = jnp.zeros((K, RHS), f32)
    for m in range(MIDS_DEV):
        own = pl.ds(8 * m, 8)
        for i in range(8):
            leaf_s[pl.ds(64 * m + i, 8, stride=8), :] = leaf_rows[own, pl.ds(i * 128, 128)].astype(f32)
        for k in range(K):
            at = 256 * m + 8 * (k % 4) + k // 4
            basis_s[pl.ds(at, 8, stride=K), :] = basis[own, pl.ds(k * M, M)].astype(f32)
        mid = four_times(unpermute(rolled_groups(mid_s[pl.ds(8 * m, 8), :])))
        lhs = [stacked_groups(leaf_s[pl.ds(64 * m + 8 * c, 8), :]) for c in range(8)]
        lhs = jnp.concatenate(lhs, axis=0).astype(bf16)
        through = jnp.dot(lhs, mid, preferred_element_type=f32)
        rows = []
        for c in range(8):
            back = through[K * c : K * (c + 1)].T[:K].astype(bf16)
            own_basis = basis_s[pl.ds(256 * m + K * c, K), :].astype(bf16)
            rows.append(jnp.dot(back, own_basis, preferred_element_type=f32))
        for h in range(2):
            four = jnp.concatenate(rows[4 * h : 4 * h + 4], axis=0)
            v_rows[2 * m + h] = four.T.astype(bf16)
        across = jnp.concatenate([row.astype(bf16) for row in rows], axis=1)
        coeffs = coeffs + jnp.dot(
            across, q[pl.ds(8 * m * M, 8 * M)], preferred_element_type=f32
        )
    whole = jnp.concatenate([coeffs, lift, lift_t], axis=0).astype(bf16)

    def put(d, carry):
        message[d] = whole
        return carry

    lax.fori_loop(0, CHIPS, put, 0, unroll=8)
    bulk.wait()
    tail.wait()


def couple_kernel(
    core, table, sources, top_target, top_source, mine, other, block_rows, top_block_rows, out,
    gathered, top_sum, top_rows, tiles_s, top_s, sems,
):
    me = core[0]
    copies = [
        pltpu.make_async_copy(mine, gathered.at[pl.ds(me * CHIPS, CHIPS)], sems.at[0]),
        pltpu.make_async_copy(other, gathered.at[pl.ds((1 - me) * CHIPS, CHIPS)], sems.at[1]),
    ]
    for copy in copies:
        copy.start()
    for i in range(8):
        piece = pl.ds(i * 128, 128)
        top_s[pl.ds(i, TOPB_DEV, stride=8), :] = top_block_rows[:, piece].astype(f32)
        for b in range(0, BLK_DEV, 8):
            n = min(8, BLK_DEV - b)
            tiles_s[pl.ds(8 * b + i, n, stride=8), :] = block_rows[pl.ds(b, n), piece].astype(f32)
    tiles_s[pl.ds(8 * BLK_DEV, 8), :] = jnp.zeros((8, 128), f32)
    for copy in copies:
        copy.wait()

    top_sum[...] = jnp.zeros((NTOP, K, RHS), f32)
    lifted = []
    for b in range(TOPB_DEV):
        source = top_source[b]
        lhs, rhs = [], []
        for c in range(8):
            child = gathered[(c % 2) * CHIPS + source * 4 + c // 2]
            lhs.append(stacked_groups(child[40:48]))
            rhs.append(four_times(child[:K]))
        lifted.append(
            jnp.dot(
                jnp.concatenate(lhs, axis=1).astype(bf16),
                jnp.concatenate(rhs, axis=0),
                preferred_element_type=f32,
            ).astype(bf16)
        )
    products = [
        jnp.dot(
            stacked_groups(top_s[pl.ds(8 * b, 8), :]).astype(bf16),
            four_times(lifted[b]),
            preferred_element_type=f32,
        )
        for b in range(TOPB_DEV)
    ]
    for b in range(TOPB_DEV):
        target = top_target[b]
        top_sum[target] = top_sum[target] + products[b]
    every = jnp.concatenate([top_sum[t] for t in range(NTOP)], axis=1)
    every = unpermute(every)
    for t in range(NTOP):
        top_rows[t] = every[:, t * RHS : (t + 1) * RHS]

    def one(d, carry):
        lhs, rhs = [], []
        for row in (0, 1):
            b = table[row, d]
            s = sources[jnp.minimum(b, BLK_DEV - 1)]
            lhs.append(stacked_groups(tiles_s[pl.ds(pl.multiple_of(8 * b, 8), 8), :]))
            rhs.append(four_times(gathered[(s % 2) * CHIPS + s // 2, :K]))
        lhs.append(stacked_groups(gathered[(d % 2) * CHIPS + d // 2, 32:40]))
        rhs.append(four_times(top_rows[d // 8]))
        out[d] = jnp.dot(
            jnp.concatenate(lhs, axis=1).astype(bf16),
            jnp.concatenate(rhs, axis=0),
            preferred_element_type=f32,
        ).astype(bf16)
        return carry

    lax.fori_loop(0, NBASE, one, 0, unroll=16)


def pieces(values):
    high = values.astype(bf16).astype(f32)
    rest = values - high
    middle = rest.astype(bf16).astype(f32)
    low = (rest - middle).astype(bf16).astype(f32)
    return high, middle, low


def features(points, source):
    row = lax.broadcasted_iota(jnp.int32, (8, M), 0)
    padded = jnp.concatenate([points, jnp.zeros((5, M), f32)], axis=0)
    centred = jnp.where(row < 3, (padded - 0.5) * math.sqrt(near_scale_sq), 0.0)
    norm = jnp.sum(centred * centred, axis=0, keepdims=True)
    if source:
        norm = norm + delta_sq * near_scale_sq
    norm = jnp.broadcast_to(norm, (8, M))
    high, middle, low = pieces(centred)
    norms = pieces(norm)
    one = jnp.ones((8, M), f32)
    if source:
        groups = [high, middle, high, low, high, middle]
    else:
        groups = [-2 * high, -2 * high, -2 * middle, -2 * high, -2 * low, -2 * middle]
    done = []
    for i, part in enumerate(groups):
        if i < 3:
            third, fourth = (one, norms[i]) if source else (norms[i], one)
            part = jnp.where(row == 3, third, jnp.where(row == 4, fourth, part))
        done.append(part)
    return jnp.concatenate(done, axis=0)


def early_kernel(near_leaves, base_target, coords, columns, table, feats, aims, named_s):
    L = LEAVES_DEV
    named_s[:, pl.ds(0, NNEAR)] = near_leaves[...]
    named = named_s[...]
    lane = lax.broadcasted_iota(jnp.int32, (L, 128), 1)
    valid = lane < NNEAR
    own = valid & (named >= L) & (named < 2 * L)
    earlier = lax.broadcasted_iota(jnp.int32, (128, 128), 0) < lax.broadcasted_iota(jnp.int32, (128, 128), 1)
    rank = jnp.dot(
        jnp.where(own, 1.0, 0.0).astype(bf16),
        jnp.where(earlier, 1.0, 0.0).astype(bf16),
        preferred_element_type=f32,
    ).astype(jnp.int32)
    count = jnp.sum(jnp.where(own, 1, 0), axis=1, keepdims=True)
    taken = own & (rank < OWN)
    place = jnp.where(taken, rank, OWN + lane - jnp.minimum(rank, OWN))
    place = jnp.where(valid, place, -1)
    value = jnp.where(taken, named - L, named)
    ordered = jnp.where(lane < OWN, L, 3 * L)
    for j in range(NNEAR):
        ordered = jnp.where(lane == place[:, j : j + 1], value[:, j : j + 1], ordered)
    columns[...] = ordered

    pairs = (OWN - jnp.minimum(count, OWN) + 1) // 2
    wide = jnp.broadcast_to(pairs, (L, 128))
    upto = lax.broadcasted_iota(jnp.int32, (L, L), 1) <= lax.broadcasted_iota(jnp.int32, (L, L), 0)
    ends = jnp.dot(
        jnp.where(upto, 1.0, 0.0).astype(bf16), wide.astype(f32).astype(bf16), preferred_element_type=f32
    ).astype(jnp.int32)
    total = jnp.sum(wide, axis=0, keepdims=True)
    table[...] = jnp.zeros((8, 256), jnp.int32)
    for block in range(2):
        unit = lane + 128 * block
        passed = ends <= unit
        leaf = jnp.sum(jnp.where(passed, 1, 0), axis=0, keepdims=True)
        slot = unit[:1] - jnp.sum(jnp.where(passed, wide, 0), axis=0, keepdims=True)
        code = jnp.where(unit[:1] < total, leaf * 64 + NNEAR + 2 * slot, SPARE)
        table[2:3, pl.ds(128 * block, 128)] = code
    table[3:4, pl.ds(0, 128)] = total

    block = lax.broadcasted_iota(jnp.int32, (NBASE, BLK_DEV), 1)
    here = base_target[...] == lax.broadcasted_iota(jnp.int32, (NBASE, BLK_DEV), 0)
    first = jnp.min(jnp.where(here, block, BLK_DEV), axis=1, keepdims=True)
    last = jnp.max(jnp.where(here, block, -1), axis=1, keepdims=True)
    second = jnp.where(last > first, last, BLK_DEV)
    for row, slot in enumerate((first, second)):
        turned = jnp.broadcast_to(slot.astype(f32), (NBASE, 128)).T
        table[row : row + 1, pl.ds(0, 128)] = turned[0:1].astype(jnp.int32)

    def prepare(g, carry):
        points = coords[:, pl.ds(pl.multiple_of(g * M, M), M)]
        feats[g] = features(points, True).astype(bf16)
        aims[g] = features(points, False).astype(bf16)
        return carry

    lax.fori_loop(0, LEAVES_DEV, prepare, 0, unroll=8)


def near_leaves_loop(first, number, columns, feats, aims, pool, done, out, kernel_a, kernel_b, sem, add):
    L = LEAVES_DEV

    def weigh(l, store):
        mine = aims[l]
        for j in range(0, number, 2):
            named = [columns[l, first + k] for k in range(j, min(j + 2, number))]
            theirs = jnp.concatenate([feats[g] for g in named], axis=1)
            squares = lax.dot_general(
                mine, theirs, (((0,), (0,)), ((), ())), preferred_element_type=f32
            )
            store[:, pl.ds(j * M, len(named) * M)] = lax.rsqrt(squares).astype(bf16)

    def apply(l, store):
        starts = [pl.multiple_of(columns[l, first + j] * M, M) for j in range(number)]
        named = jnp.concatenate([pool[pl.ds(start, M)] for start in starts], axis=0)
        field = jnp.dot(store[...], named, preferred_element_type=f32)
        done[l] = done[l] + field if add else field

    weigh(0, kernel_a)

    def eight(i, carry):
        for l in range(0, 8, 2):
            weigh(8 * i + l + 1, kernel_b)
            apply(8 * i + l, kernel_a)
            weigh(jnp.minimum(8 * i + l + 2, L - 1), kernel_a)
            apply(8 * i + l + 1, kernel_b)
        part = pl.ds(8 * i, 8)
        pltpu.make_async_copy(done.at[part], out.at[part], sem).start()
        return carry

    lax.fori_loop(0, L // 8, eight, 0)
    pltpu.make_async_copy(done, out, sem).wait()


def own_kernel(columns, own_feats, own_aims, charges, out, pool, feats, aims, kernel_a, kernel_b, done, sems):
    L = LEAVES_DEV
    copies = [
        pltpu.make_async_copy(own_aims, aims, sems.at[0]),
        pltpu.make_async_copy(own_feats, feats.at[pl.ds(0, L)], sems.at[1]),
        pltpu.make_async_copy(charges, pool.at[pl.ds(0, POINTS)], sems.at[2]),
    ]
    for copy in copies:
        copy.start()
    pool[pl.ds(POINTS, M)] = jnp.zeros((M, RHS), bf16)
    for copy in copies:
        copy.wait()
    feats[L] = feats[0]

    def weigh(batch, store):
        for u in range(8):
            l = jnp.minimum(8 * batch + u, L - 1)
            for j in range(0, OWN, 2):
                theirs = jnp.concatenate([feats[columns[l, j]], feats[columns[l, j + 1]]], axis=1)
                squares = lax.dot_general(
                    aims[l], theirs, (((0,), (0,)), ((), ())), preferred_element_type=f32
                )
                store[u, :, pl.ds(j * M, 2 * M)] = lax.rsqrt(squares).astype(bf16)

    def apply(batch, store):
        for u in range(8):
            l = 8 * batch + u
            starts = [pl.multiple_of(columns[l, j] * M, M) for j in range(OWN)]
            named = jnp.concatenate([pool[pl.ds(start, M)] for start in starts], axis=0)
            done[l] = jnp.dot(store[u], named, preferred_element_type=f32)
        part = pl.ds(8 * batch, 8)
        pltpu.make_async_copy(done.at[part], out.at[part], sems.at[3]).start()

    weigh(0, kernel_a)

    def two(i, carry):
        weigh(2 * i + 1, kernel_b)
        apply(2 * i, kernel_a)
        weigh(2 * i + 2, kernel_a)
        apply(2 * i + 1, kernel_b)
        return carry

    lax.fori_loop(0, L // 16, two, 0)
    pltpu.make_async_copy(done, out, sems.at[3]).wait()


def near_kernel(
    columns, table, own_feats, own_aims, before, own, after, so_far, out,
    pool, feats, aims, tails, points_s, kernel_a, kernel_b, units_a, units_b, done, sems,
):
    L = LEAVES_DEV
    tail_copies = [
        pltpu.make_async_copy(part.at[pl.ds(POINTS, TAIL)], tails.at[i], sems.at[i])
        for i, part in enumerate((before, after))
    ]
    copies = [
        pltpu.make_async_copy(own_aims, aims, sems.at[2]),
        pltpu.make_async_copy(own_feats, feats.at[pl.ds(L, L)], sems.at[3]),
    ]
    copies += [
        pltpu.make_async_copy(
            part.at[pl.ds(0, POINTS)], pool.at[pl.ds(i * POINTS, POINTS)], sems.at[4 + i]
        )
        for i, part in enumerate((before, own, after))
    ]
    copies.append(pltpu.make_async_copy(so_far, done, sems.at[7]))
    for copy in tail_copies + copies:
        copy.start()
    pool[pl.ds(3 * POINTS, M)] = jnp.zeros((M, RHS), bf16)
    for i in range(2):
        tail_copies[i].wait()
        part = [tails[i, pl.ds(p * 3 * L, 3 * L)].astype(f32) for p in range(3)]
        points_s[i] = part[0] + part[1] + part[2]

        def prepare(g, carry, i=i):
            points = points_s[i, pl.ds(g, 3, stride=L), :]
            feats[2 * i * L + g] = features(points, True).astype(bf16)
            return carry

        lax.fori_loop(0, L, prepare, 0, unroll=8)
    feats[3 * L] = feats[0]
    for copy in copies:
        copy.wait()

    def unit(v):
        code = table[2, v]
        leaf, slot = code // 64, code % 64
        return leaf, columns[leaf, slot], columns[leaf, slot + 1]

    def weigh(batch, store):
        for u in range(UNITS):
            leaf, g, h = unit(batch * UNITS + u)
            theirs = jnp.concatenate([feats[g], feats[h]], axis=1)
            squares = lax.dot_general(
                aims[leaf], theirs, (((0,), (0,)), ((), ())), preferred_element_type=f32
            )
            store[u] = lax.rsqrt(squares).astype(bf16)

    def apply(batch, store):
        for u in range(UNITS):
            leaf, g, h = unit(batch * UNITS + u)
            starts = [pl.multiple_of(k * M, M) for k in (g, h)]
            named = jnp.concatenate([pool[pl.ds(start, M)] for start in starts], axis=0)
            done[leaf] = done[leaf] + jnp.dot(store[u], named, preferred_element_type=f32)

    def two(i, carry):
        weigh(2 * i, units_a)
        weigh(2 * i + 1, units_b)
        apply(2 * i, units_a)
        apply(2 * i + 1, units_b)
        return carry

    lax.fori_loop(0, (table[3, 0] + 2 * UNITS - 1) // (2 * UNITS), two, 0)
    near_leaves_loop(
        OWN, REST, columns, feats, aims, pool, done, out, kernel_a, kernel_b, sems.at[8], True
    )


def down_kernel(parts, v_rows, near, out, v_s, near_s, out_s, sems):
    steps = LEAVES_DEV // 8
    chunks = [pl.ds(8 * i, 8) for i in range(steps)]
    first = [
        pltpu.make_async_copy(v_rows, v_s, sems.at[1]),
    ]
    loads = [
        pltpu.make_async_copy(near.at[c], near_s.at[c], sems.at[2 + i])
        for i, c in enumerate(chunks)
    ]
    for copy in first + loads:
        copy.start()
    to = lax.broadcasted_iota(jnp.int32, (K, NBASE * K), 0)
    at = lax.broadcasted_iota(jnp.int32, (K, NBASE * K), 1) % K
    order = jnp.where(to == 4 * (at % 8) + at // 8, 1.0, 0.0).astype(bf16)
    field = jnp.dot(order, parts[...].reshape(NBASE * K, RHS), preferred_element_type=f32)
    zero = jnp.zeros((K, RHS), f32)
    spread = [
        jnp.concatenate([field if g == h else zero for h in range(4)], axis=0) for g in range(4)
    ]
    spread = jnp.concatenate(spread, axis=1).astype(bf16)
    first[0].wait()
    stores = []
    for i, chunk in enumerate(chunks):
        rows = v_s[pl.ds(2 * i, 2)].reshape(2 * M, 4 * K)
        far = jnp.dot(rows, spread, preferred_element_type=f32)
        loads[i].wait()
        for c in range(8):
            h, g = c // 4, c % 4
            part = far[h * M : (h + 1) * M, g * RHS : (g + 1) * RHS]
            out_s[8 * i + c] = (near_s[8 * i + c] + part).astype(bf16)
        stores.append(pltpu.make_async_copy(out_s.at[chunk], out.at[chunk], sems.at[10 + i]))
        stores[-1].start()
    for copy in stores:
        copy.wait()


def all_steps(
    coords, charges, near_leaves, leaf_basis, leaf_transfer, mid_transfer, base_transfer,
    base_coupling, base_target, base_source, top_coupling, top_target, top_source,
):
    L = LEAVES_DEV
    size = lax.axis_size(LEAF)
    up = [(i, i + 1) for i in range(size - 1)]
    down = [(j, i) for i, j in up]
    message, v_rows, halo = pl.pallas_call(
        up_kernel,
        out_shape=(
            jax.ShapeDtypeStruct((CHIPS, MSG, RHS), bf16),
            jax.ShapeDtypeStruct((L // 4, M, 4 * K), bf16),
            jax.ShapeDtypeStruct((POINTS + TAIL, RHS), bf16),
        ),
        in_specs=[in_vmem()] * 6,
        out_specs=(in_vmem(), in_vmem(), in_place()),
        scratch_shapes=[
            pltpu.VMEM((L * K, M), f32),
            pltpu.VMEM((L * 8, 128), f32),
            pltpu.VMEM((MIDS_DEV * 8, 128), f32),
            pltpu.VMEM((8, 128), f32),
            pltpu.VMEM((3 * L, M), f32),
            pltpu.VMEM((TAIL, M), bf16),
            pltpu.SemaphoreType.DMA((2,)),
        ],
        name="up",
        cost_estimate=pl.CostEstimate(flops=2 * 10**9, bytes_accessed=5 * 10**6, transcendentals=0),
    )(charges, coords, leaf_basis, leaf_transfer, mid_transfer, base_transfer)
    mine = lax.all_to_all(message, LEAF[:3], 0, 0, tiled=True)
    other = lax.ppermute(mine, LEAF[3], [(0, 1), (1, 0)])
    before = lax.ppermute(halo, LEAF, up)
    after = lax.ppermute(halo, LEAF, down)

    columns, table, own_feats, own_aims = pl.pallas_call(
        early_kernel,
        out_shape=(
            jax.ShapeDtypeStruct((L, 128), jnp.int32),
            jax.ShapeDtypeStruct((8, 256), jnp.int32),
            jax.ShapeDtypeStruct((L, FEAT, M), bf16),
            jax.ShapeDtypeStruct((L, FEAT, M), bf16),
        ),
        in_specs=[in_vmem()] * 3,
        out_specs=(in_vmem(),) * 4,
        scratch_shapes=[pltpu.VMEM((L, 128), jnp.int32)],
        name="early",
        cost_estimate=pl.CostEstimate(flops=10**9, bytes_accessed=10**6, transcendentals=0),
    )(
        near_leaves,
        base_target.reshape(1, BLK_DEV),
        coords,
    )

    mine = pltpu.with_memory_space_constraint(mine, pltpu.VMEM)
    other = pltpu.with_memory_space_constraint(other, pltpu.VMEM)
    partial = pl.pallas_call(
        couple_kernel,
        out_shape=jax.ShapeDtypeStruct((NBASE, K, RHS), bf16),
        in_specs=[in_smem()] * 5 + [in_vmem()] * 4,
        out_specs=in_vmem(),
        scratch_shapes=[
            pltpu.VMEM((NBASE, MSG, RHS), bf16),
            pltpu.VMEM((NTOP, K, RHS), f32),
            pltpu.VMEM((NTOP, K, RHS), bf16),
            pltpu.VMEM((8 * BLK_DEV + 8, 128), f32),
            pltpu.VMEM((8 * TOPB_DEV, 128), f32),
            pltpu.SemaphoreType.DMA((2,)),
        ],
        name="couple",
        cost_estimate=pl.CostEstimate(flops=2 * 10**9, bytes_accessed=5 * 10**6, transcendentals=0),
    )(
        lax.axis_index(LEAF[3]).reshape(1).astype(jnp.int32),
        table,
        base_source,
        top_target,
        top_source,
        mine,
        other,
        base_coupling,
        top_coupling,
    )
    parts = lax.all_to_all(partial, LEAF, 0, 0, tiled=True)

    near_own = pl.pallas_call(
        own_kernel,
        out_shape=jax.ShapeDtypeStruct((L, M, RHS), f32),
        in_specs=[in_smem()] + [in_place()] * 3,
        out_specs=in_place(),
        scratch_shapes=[
            pltpu.VMEM((POINTS + M, RHS), bf16),
            pltpu.VMEM((L + 1, FEAT, M), bf16),
            pltpu.VMEM((L, FEAT, M), bf16),
            pltpu.VMEM((8, M, OWN * M), bf16),
            pltpu.VMEM((8, M, OWN * M), bf16),
            pltpu.VMEM((L, M, RHS), f32),
            pltpu.SemaphoreType.DMA((4,)),
        ],
        name="own",
        cost_estimate=pl.CostEstimate(
            flops=10**10, bytes_accessed=10**7, transcendentals=7 * 10**6
        ),
    )(columns, own_feats, own_aims, charges)
    near = pl.pallas_call(
        near_kernel,
        out_shape=jax.ShapeDtypeStruct((L, M, RHS), f32),
        in_specs=[in_smem()] * 2 + [in_place()] * 6,
        out_specs=in_place(),
        scratch_shapes=[
            pltpu.VMEM((3 * POINTS + M, RHS), bf16),
            pltpu.VMEM((3 * L + 1, FEAT, M), bf16),
            pltpu.VMEM((L, FEAT, M), bf16),
            pltpu.VMEM((2, TAIL, M), bf16),
            pltpu.VMEM((2, 3 * L, M), f32),
            pltpu.VMEM((M, REST * M), bf16),
            pltpu.VMEM((M, REST * M), bf16),
            pltpu.VMEM((UNITS, M, 2 * M), bf16),
            pltpu.VMEM((UNITS, M, 2 * M), bf16),
            pltpu.VMEM((L, M, RHS), f32),
            pltpu.SemaphoreType.DMA((9,)),
        ],
        name="near",
        cost_estimate=pl.CostEstimate(
            flops=4 * 10**10, bytes_accessed=10**7, transcendentals=3 * 10**7
        ),
    )(columns, table, own_feats, own_aims, before, charges, after, near_own)

    potential = pl.pallas_call(
        down_kernel,
        out_shape=jax.ShapeDtypeStruct((L, M, RHS), bf16),
        in_specs=[in_vmem()] + [in_place()] * 2,
        out_specs=in_place(),
        scratch_shapes=[
            pltpu.VMEM((L // 4, M, 4 * K), bf16),
            pltpu.VMEM((L, M, RHS), f32),
            pltpu.VMEM((L, M, RHS), bf16),
            pltpu.SemaphoreType.DMA((18,)),
        ],
        name="down",
        cost_estimate=pl.CostEstimate(flops=10**9, bytes_accessed=10**7, transcendentals=0),
    )(pltpu.with_memory_space_constraint(parts, pltpu.VMEM), v_rows, near)
    return potential.reshape(L * M, RHS)


def solution(mesh):
    split = Mesh(mesh.devices.reshape(4, 4, 4, 2), LEAF)
    by_leaf = P(LEAF, None)
    in_specs = (P(None, LEAF),) + (by_leaf,) * 8 + (P(LEAF), by_leaf, P(LEAF), P(LEAF))
    return jax.shard_map(
        all_steps, mesh=split, in_specs=in_specs, out_specs=by_leaf, check_vma=False
    )
```

```python
import math

import jax
import jax.numpy as jnp
from jax import lax
from jax.experimental import pallas as pl
from jax.experimental.pallas import tpu as pltpu
from jax.sharding import Mesh
from jax.sharding import PartitionSpec as P

K = 32
RHS = 128
M = 128
NNEAR = 27
LEAVES_DEV = 64
MIDS_DEV = 8
NBASE = 128
CHIPS = 64
NTOP = 16
BLK_DEV = 189
TOPB_DEV = 8
FEAT = 48
OWN = 6
REST = NNEAR - OWN
UNITS = 4
BATCH = 4
SPARE = 40
POINTS = 8192
TAIL = 576
MSG = 48
LEAF = ("leaf_0", "leaf_1", "leaf_2", "leaf_3")
delta_sq = 0.0025
near_scale_sq = float(NNEAR * M)

f32 = jnp.float32
bf16 = jnp.bfloat16


def in_vmem():
    return pl.BlockSpec(memory_space=pltpu.VMEM)


def in_smem():
    return pl.BlockSpec(memory_space=pltpu.SMEM)


def in_place():
    return pl.BlockSpec(memory_space=pl.ANY)


def stacked_groups(tile):
    tile = tile.astype(f32)
    group = lax.broadcasted_iota(jnp.int32, tile.shape, 1) // K
    return jnp.concatenate([jnp.where(group == g, tile, 0.0) for g in range(4)], axis=0)


def rolled_groups(tile):
    tile = tile.astype(f32)
    lane = lax.broadcasted_iota(jnp.int32, tile.shape, 1)
    parts = [tile] + [pltpu.roll(tile, 128 - K * g, 1) for g in range(1, 4)]
    return jnp.concatenate([jnp.where(lane < K, part, 0.0) for part in parts], axis=0)


def unpermute(rows):
    to = lax.broadcasted_iota(jnp.int32, (K, K), 0)
    at = lax.broadcasted_iota(jnp.int32, (K, K), 1)
    order = jnp.where(to == 4 * (at % 8) + at // 8, 1.0, 0.0).astype(bf16)
    return jnp.dot(order, rows.astype(bf16), preferred_element_type=f32).astype(bf16)


def four_times(rows):
    return jnp.concatenate([rows] * 4, axis=0)


def up_kernel(
    q, coords, basis, leaf_rows, mid_rows, lift_rows, message, v_rows, halo,
    basis_s, leaf_s, mid_s, lift_s, points_s, tail_s, sems,
):
    bulk = pltpu.make_async_copy(q, halo.at[pl.ds(0, POINTS)], sems.at[0])
    bulk.start()

    def spread(g, carry):
        row = coords[:, pl.ds(pl.multiple_of(g * M, M), M)]
        points_s[pl.ds(g, 3, stride=LEAVES_DEV), :] = row
        return carry

    lax.fori_loop(0, LEAVES_DEV, spread, 0, unroll=8)
    for i, piece in enumerate(pieces(points_s[...])):
        tail_s[pl.ds(i * 3 * LEAVES_DEV, 3 * LEAVES_DEV), :] = piece.astype(bf16)
    tail = pltpu.make_async_copy(tail_s, halo.at[pl.ds(POINTS, TAIL)], sems.at[1])
    tail.start()

    for i in range(8):
        piece = pl.ds(i * 128, 128)
        mid_s[pl.ds(i, MIDS_DEV, stride=8), :] = mid_rows[:, piece].astype(f32)
        lift_s[pl.ds(i, 1), :] = lift_rows[:, piece].astype(f32)
    lift = lift_s[pl.ds(0, 8), :]
    straight = unpermute(rolled_groups(lift)).astype(f32)
    turned = jnp.concatenate([straight, jnp.zeros((96, 128), f32)], axis=0).T
    lift_t = turned[:8]
    for g in range(1, 4):
        lift_t = lift_t + pltpu.roll(turned[8 * g : 8 * g + 8], K * g, 1)

    coeffs = jnp.zeros((K, RHS), f32)
    for m in range(MIDS_DEV):
        own = pl.ds(8 * m, 8)
        for i in range(8):
            leaf_s[pl.ds(64 * m + i, 8, stride=8), :] = leaf_rows[own, pl.ds(i * 128, 128)].astype(f32)
        for k in range(K):
            at = 256 * m + 8 * (k % 4) + k // 4
            basis_s[pl.ds(at, 8, stride=K), :] = basis[own, pl.ds(k * M, M)].astype(f32)
        mid = four_times(unpermute(rolled_groups(mid_s[pl.ds(8 * m, 8), :])))
        lhs = [stacked_groups(leaf_s[pl.ds(64 * m + 8 * c, 8), :]) for c in range(8)]
        lhs = jnp.concatenate(lhs, axis=0).astype(bf16)
        through = jnp.dot(lhs, mid, preferred_element_type=f32)
        rows = []
        for c in range(8):
            back = through[K * c : K * (c + 1)].T[:K].astype(bf16)
            own_basis = basis_s[pl.ds(256 * m + K * c, K), :].astype(bf16)
            rows.append(jnp.dot(back, own_basis, preferred_element_type=f32))
        for h in range(2):
            four = jnp.concatenate(rows[4 * h : 4 * h + 4], axis=0)
            v_rows[2 * m + h] = four.T.astype(bf16)
        across = jnp.concatenate([row.astype(bf16) for row in rows], axis=1)
        coeffs = coeffs + jnp.dot(
            across, q[pl.ds(8 * m * M, 8 * M)], preferred_element_type=f32
        )
    whole = jnp.concatenate([coeffs, lift, lift_t], axis=0).astype(bf16)

    def put(d, carry):
        message[d] = whole
        return carry

    lax.fori_loop(0, CHIPS, put, 0, unroll=8)
    bulk.wait()
    tail.wait()


def couple_kernel(
    core, table, sources, top_target, top_source, mine, other, block_rows, top_block_rows, out,
    gathered, top_sum, top_rows, tiles_s, top_s, sems,
):
    me = core[0]
    copies = [
        pltpu.make_async_copy(mine, gathered.at[pl.ds(me * CHIPS, CHIPS)], sems.at[0]),
        pltpu.make_async_copy(other, gathered.at[pl.ds((1 - me) * CHIPS, CHIPS)], sems.at[1]),
    ]
    for copy in copies:
        copy.start()
    for i in range(8):
        piece = pl.ds(i * 128, 128)
        top_s[pl.ds(i, TOPB_DEV, stride=8), :] = top_block_rows[:, piece].astype(f32)
        for b in range(0, BLK_DEV, 8):
            n = min(8, BLK_DEV - b)
            tiles_s[pl.ds(8 * b + i, n, stride=8), :] = block_rows[pl.ds(b, n), piece].astype(f32)
    tiles_s[pl.ds(8 * BLK_DEV, 8), :] = jnp.zeros((8, 128), f32)
    for copy in copies:
        copy.wait()

    top_sum[...] = jnp.zeros((NTOP, K, RHS), f32)
    lifted = []
    for b in range(TOPB_DEV):
        source = top_source[b]
        lhs, rhs = [], []
        for c in range(8):
            child = gathered[(c % 2) * CHIPS + source * 4 + c // 2]
            lhs.append(stacked_groups(child[40:48]))
            rhs.append(four_times(child[:K]))
        lifted.append(
            jnp.dot(
                jnp.concatenate(lhs, axis=1).astype(bf16),
                jnp.concatenate(rhs, axis=0),
                preferred_element_type=f32,
            ).astype(bf16)
        )
    products = [
        jnp.dot(
            stacked_groups(top_s[pl.ds(8 * b, 8), :]).astype(bf16),
            four_times(lifted[b]),
            preferred_element_type=f32,
        )
        for b in range(TOPB_DEV)
    ]
    for b in range(TOPB_DEV):
        target = top_target[b]
        top_sum[target] = top_sum[target] + products[b]
    every = jnp.concatenate([top_sum[t] for t in range(NTOP)], axis=1)
    every = unpermute(every)
    for t in range(NTOP):
        top_rows[t] = every[:, t * RHS : (t + 1) * RHS]

    def one(d, carry):
        lhs, rhs = [], []
        for row in (0, 1):
            b = table[row, d]
            s = sources[jnp.minimum(b, BLK_DEV - 1)]
            lhs.append(stacked_groups(tiles_s[pl.ds(pl.multiple_of(8 * b, 8), 8), :]))
            rhs.append(four_times(gathered[(s % 2) * CHIPS + s // 2, :K]))
        lhs.append(stacked_groups(gathered[(d % 2) * CHIPS + d // 2, 32:40]))
        rhs.append(four_times(top_rows[d // 8]))
        out[d] = jnp.dot(
            jnp.concatenate(lhs, axis=1).astype(bf16),
            jnp.concatenate(rhs, axis=0),
            preferred_element_type=f32,
        ).astype(bf16)
        return carry

    lax.fori_loop(0, NBASE, one, 0, unroll=16)


def pieces(values):
    high = values.astype(bf16).astype(f32)
    rest = values - high
    middle = rest.astype(bf16).astype(f32)
    low = (rest - middle).astype(bf16).astype(f32)
    return high, middle, low


def features(points, source):
    row = lax.broadcasted_iota(jnp.int32, (8, M), 0)
    padded = jnp.concatenate([points, jnp.zeros((5, M), f32)], axis=0)
    centred = jnp.where(row < 3, (padded - 0.5) * math.sqrt(near_scale_sq), 0.0)
    norm = jnp.sum(centred * centred, axis=0, keepdims=True)
    if source:
        norm = norm + delta_sq * near_scale_sq
    norm = jnp.broadcast_to(norm, (8, M))
    high, middle, low = pieces(centred)
    norms = pieces(norm)
    one = jnp.ones((8, M), f32)
    if source:
        groups = [high, middle, high, low, high, middle]
    else:
        groups = [-2 * high, -2 * high, -2 * middle, -2 * high, -2 * low, -2 * middle]
    done = []
    for i, part in enumerate(groups):
        if i < 3:
            third, fourth = (one, norms[i]) if source else (norms[i], one)
            part = jnp.where(row == 3, third, jnp.where(row == 4, fourth, part))
        done.append(part)
    return jnp.concatenate(done, axis=0)


def early_kernel(near_leaves, base_target, coords, columns, table, feats, aims, named_s):
    L = LEAVES_DEV
    named_s[:, pl.ds(0, NNEAR)] = near_leaves[...]
    named = named_s[...]
    lane = lax.broadcasted_iota(jnp.int32, (L, 128), 1)
    valid = lane < NNEAR
    own = valid & (named >= L) & (named < 2 * L)
    earlier = lax.broadcasted_iota(jnp.int32, (128, 128), 0) < lax.broadcasted_iota(jnp.int32, (128, 128), 1)
    rank = jnp.dot(
        jnp.where(own, 1.0, 0.0).astype(bf16),
        jnp.where(earlier, 1.0, 0.0).astype(bf16),
        preferred_element_type=f32,
    ).astype(jnp.int32)
    count = jnp.sum(jnp.where(own, 1, 0), axis=1, keepdims=True)
    taken = own & (rank < OWN)
    place = jnp.where(taken, rank, OWN + lane - jnp.minimum(rank, OWN))
    place = jnp.where(valid, place, -1)
    value = jnp.where(taken, named - L, named)
    ordered = jnp.where(lane < OWN, L, 3 * L)
    for j in range(NNEAR):
        ordered = jnp.where(lane == place[:, j : j + 1], value[:, j : j + 1], ordered)
    columns[...] = ordered

    pairs = (OWN - jnp.minimum(count, OWN) + 1) // 2
    wide = jnp.broadcast_to(pairs, (L, 128))
    upto = lax.broadcasted_iota(jnp.int32, (L, L), 1) <= lax.broadcasted_iota(jnp.int32, (L, L), 0)
    ends = jnp.dot(
        jnp.where(upto, 1.0, 0.0).astype(bf16), wide.astype(f32).astype(bf16), preferred_element_type=f32
    ).astype(jnp.int32)
    total = jnp.sum(wide, axis=0, keepdims=True)
    table[...] = jnp.zeros((8, 256), jnp.int32)
    for block in range(2):
        unit = lane + 128 * block
        passed = ends <= unit
        leaf = jnp.sum(jnp.where(passed, 1, 0), axis=0, keepdims=True)
        slot = unit[:1] - jnp.sum(jnp.where(passed, wide, 0), axis=0, keepdims=True)
        code = jnp.where(unit[:1] < total, leaf * 64 + NNEAR + 2 * slot, SPARE)
        table[2:3, pl.ds(128 * block, 128)] = code
    table[3:4, pl.ds(0, 128)] = total

    block = lax.broadcasted_iota(jnp.int32, (NBASE, BLK_DEV), 1)
    here = base_target[...] == lax.broadcasted_iota(jnp.int32, (NBASE, BLK_DEV), 0)
    first = jnp.min(jnp.where(here, block, BLK_DEV), axis=1, keepdims=True)
    last = jnp.max(jnp.where(here, block, -1), axis=1, keepdims=True)
    second = jnp.where(last > first, last, BLK_DEV)
    for row, slot in enumerate((first, second)):
        turned = jnp.broadcast_to(slot.astype(f32), (NBASE, 128)).T
        table[row : row + 1, pl.ds(0, 128)] = turned[0:1].astype(jnp.int32)

    def prepare(g, carry):
        points = coords[:, pl.ds(pl.multiple_of(g * M, M), M)]
        feats[g] = features(points, True).astype(bf16)
        aims[g] = features(points, False).astype(bf16)
        return carry

    lax.fori_loop(0, LEAVES_DEV, prepare, 0, unroll=8)


def near_leaves_loop(first, number, columns, feats, aims, pool, done, out, kernel_a, kernel_b, sem, add):
    L = LEAVES_DEV

    def weigh(l, store):
        mine = aims[l]
        for j in range(0, number, 2):
            named = [columns[l, first + k] for k in range(j, min(j + 2, number))]
            theirs = jnp.concatenate([feats[g] for g in named], axis=1)
            squares = lax.dot_general(
                mine, theirs, (((0,), (0,)), ((), ())), preferred_element_type=f32
            )
            store[:, pl.ds(j * M, len(named) * M)] = lax.rsqrt(squares).astype(bf16)

    def apply(l, store):
        starts = [pl.multiple_of(columns[l, first + j] * M, M) for j in range(number)]
        named = jnp.concatenate([pool[pl.ds(start, M)] for start in starts], axis=0)
        field = jnp.dot(store[...], named, preferred_element_type=f32)
        done[l] = done[l] + field if add else field

    weigh(0, kernel_a)

    def eight(i, carry):
        for l in range(0, 8, 2):
            weigh(8 * i + l + 1, kernel_b)
            apply(8 * i + l, kernel_a)
            weigh(jnp.minimum(8 * i + l + 2, L - 1), kernel_a)
            apply(8 * i + l + 1, kernel_b)
        part = pl.ds(8 * i, 8)
        pltpu.make_async_copy(done.at[part], out.at[part], sem).start()
        return carry

    lax.fori_loop(0, L // 8, eight, 0)
    pltpu.make_async_copy(done, out, sem).wait()


def own_kernel(columns, own_feats, own_aims, charges, out, pool, feats, aims, kernel_a, kernel_b, done, sems):
    L = LEAVES_DEV
    copies = [
        pltpu.make_async_copy(own_aims, aims, sems.at[0]),
        pltpu.make_async_copy(own_feats, feats.at[pl.ds(0, L)], sems.at[1]),
        pltpu.make_async_copy(charges, pool.at[pl.ds(0, POINTS)], sems.at[2]),
    ]
    for copy in copies:
        copy.start()
    pool[pl.ds(POINTS, M)] = jnp.zeros((M, RHS), bf16)
    for copy in copies:
        copy.wait()
    feats[L] = feats[0]

    def weigh(batch, store):
        for u in range(BATCH):
            l = jnp.minimum(BATCH * batch + u, L - 1)
            for j in range(0, OWN, 2):
                theirs = jnp.concatenate([feats[columns[l, j]], feats[columns[l, j + 1]]], axis=1)
                squares = lax.dot_general(
                    aims[l], theirs, (((0,), (0,)), ((), ())), preferred_element_type=f32
                )
                store[u, :, pl.ds(j * M, 2 * M)] = lax.rsqrt(squares).astype(bf16)

    def apply(batch, store):
        for u in range(BATCH):
            l = BATCH * batch + u
            starts = [pl.multiple_of(columns[l, j] * M, M) for j in range(OWN)]
            named = jnp.concatenate([pool[pl.ds(start, M)] for start in starts], axis=0)
            done[l] = jnp.dot(store[u], named, preferred_element_type=f32)
        part = pl.ds(BATCH * batch, BATCH)
        pltpu.make_async_copy(done.at[part], out.at[part], sems.at[3]).start()

    weigh(0, kernel_a)

    def two(i, carry):
        weigh(2 * i + 1, kernel_b)
        apply(2 * i, kernel_a)
        weigh(2 * i + 2, kernel_a)
        apply(2 * i + 1, kernel_b)
        return carry

    lax.fori_loop(0, L // (2 * BATCH), two, 0, unroll=2)
    pltpu.make_async_copy(done, out, sems.at[3]).wait()


def near_kernel(
    columns, table, own_feats, own_aims, before, own, after, so_far, out,
    pool, feats, aims, tails, points_s, kernel_a, kernel_b, units_a, units_b, done, sems,
):
    L = LEAVES_DEV
    tail_copies = [
        pltpu.make_async_copy(part.at[pl.ds(POINTS, TAIL)], tails.at[i], sems.at[i])
        for i, part in enumerate((before, after))
    ]
    copies = [
        pltpu.make_async_copy(own_aims, aims, sems.at[2]),
        pltpu.make_async_copy(own_feats, feats.at[pl.ds(L, L)], sems.at[3]),
    ]
    copies += [
        pltpu.make_async_copy(
            part.at[pl.ds(0, POINTS)], pool.at[pl.ds(i * POINTS, POINTS)], sems.at[4 + i]
        )
        for i, part in enumerate((before, own, after))
    ]
    copies.append(pltpu.make_async_copy(so_far, done, sems.at[7]))
    for copy in tail_copies + copies:
        copy.start()
    pool[pl.ds(3 * POINTS, M)] = jnp.zeros((M, RHS), bf16)
    for i in range(2):
        tail_copies[i].wait()
        part = [tails[i, pl.ds(p * 3 * L, 3 * L)].astype(f32) for p in range(3)]
        points_s[i] = part[0] + part[1] + part[2]

        def prepare(g, carry, i=i):
            points = points_s[i, pl.ds(g, 3, stride=L), :]
            feats[2 * i * L + g] = features(points, True).astype(bf16)
            return carry

        lax.fori_loop(0, L, prepare, 0, unroll=8)
    feats[3 * L] = feats[0]
    for copy in copies:
        copy.wait()

    def unit(v):
        code = table[2, v]
        leaf, slot = code // 64, code % 64
        return leaf, columns[leaf, slot], columns[leaf, slot + 1]

    def weigh(batch, store):
        for u in range(UNITS):
            leaf, g, h = unit(batch * UNITS + u)
            theirs = jnp.concatenate([feats[g], feats[h]], axis=1)
            squares = lax.dot_general(
                aims[leaf], theirs, (((0,), (0,)), ((), ())), preferred_element_type=f32
            )
            store[u] = lax.rsqrt(squares).astype(bf16)

    def apply(batch, store):
        for u in range(UNITS):
            leaf, g, h = unit(batch * UNITS + u)
            starts = [pl.multiple_of(k * M, M) for k in (g, h)]
            named = jnp.concatenate([pool[pl.ds(start, M)] for start in starts], axis=0)
            done[leaf] = done[leaf] + jnp.dot(store[u], named, preferred_element_type=f32)

    def two(i, carry):
        weigh(2 * i, units_a)
        weigh(2 * i + 1, units_b)
        apply(2 * i, units_a)
        apply(2 * i + 1, units_b)
        return carry

    lax.fori_loop(0, (table[3, 0] + 2 * UNITS - 1) // (2 * UNITS), two, 0)
    near_leaves_loop(
        OWN, REST, columns, feats, aims, pool, done, out, kernel_a, kernel_b, sems.at[8], True
    )


def down_kernel(parts, v_rows, near, out, v_s, near_s, out_s, sems):
    steps = LEAVES_DEV // 8
    chunks = [pl.ds(8 * i, 8) for i in range(steps)]
    first = [
        pltpu.make_async_copy(v_rows, v_s, sems.at[1]),
    ]
    loads = [
        pltpu.make_async_copy(near.at[c], near_s.at[c], sems.at[2 + i])
        for i, c in enumerate(chunks)
    ]
    for copy in first + loads:
        copy.start()
    to = lax.broadcasted_iota(jnp.int32, (K, NBASE * K), 0)
    at = lax.broadcasted_iota(jnp.int32, (K, NBASE * K), 1) % K
    order = jnp.where(to == 4 * (at % 8) + at // 8, 1.0, 0.0).astype(bf16)
    field = jnp.dot(order, parts[...].reshape(NBASE * K, RHS), preferred_element_type=f32)
    zero = jnp.zeros((K, RHS), f32)
    spread = [
        jnp.concatenate([field if g == h else zero for h in range(4)], axis=0) for g in range(4)
    ]
    spread = jnp.concatenate(spread, axis=1).astype(bf16)
    first[0].wait()
    stores = []
    for i, chunk in enumerate(chunks):
        rows = v_s[pl.ds(2 * i, 2)].reshape(2 * M, 4 * K)
        far = jnp.dot(rows, spread, preferred_element_type=f32)
        loads[i].wait()
        for c in range(8):
            h, g = c // 4, c % 4
            part = far[h * M : (h + 1) * M, g * RHS : (g + 1) * RHS]
            out_s[8 * i + c] = (near_s[8 * i + c] + part).astype(bf16)
        stores.append(pltpu.make_async_copy(out_s.at[chunk], out.at[chunk], sems.at[10 + i]))
        stores[-1].start()
    for copy in stores:
        copy.wait()


def all_steps(
    coords, charges, near_leaves, leaf_basis, leaf_transfer, mid_transfer, base_transfer,
    base_coupling, base_target, base_source, top_coupling, top_target, top_source,
):
    L = LEAVES_DEV
    size = lax.axis_size(LEAF)
    up = [(i, i + 1) for i in range(size - 1)]
    down = [(j, i) for i, j in up]
    message, v_rows, halo = pl.pallas_call(
        up_kernel,
        out_shape=(
            jax.ShapeDtypeStruct((CHIPS, MSG, RHS), bf16),
            jax.ShapeDtypeStruct((L // 4, M, 4 * K), bf16),
            jax.ShapeDtypeStruct((POINTS + TAIL, RHS), bf16),
        ),
        in_specs=[in_vmem()] * 6,
        out_specs=(in_vmem(), in_vmem(), in_place()),
        scratch_shapes=[
            pltpu.VMEM((L * K, M), f32),
            pltpu.VMEM((L * 8, 128), f32),
            pltpu.VMEM((MIDS_DEV * 8, 128), f32),
            pltpu.VMEM((8, 128), f32),
            pltpu.VMEM((3 * L, M), f32),
            pltpu.VMEM((TAIL, M), bf16),
            pltpu.SemaphoreType.DMA((2,)),
        ],
        name="up",
        cost_estimate=pl.CostEstimate(flops=2 * 10**9, bytes_accessed=5 * 10**6, transcendentals=0),
    )(charges, coords, leaf_basis, leaf_transfer, mid_transfer, base_transfer)
    mine = lax.all_to_all(message, LEAF[:3], 0, 0, tiled=True)
    other = lax.ppermute(mine, LEAF[3], [(0, 1), (1, 0)])
    before = lax.ppermute(halo, LEAF, up)
    after = lax.ppermute(halo, LEAF, down)

    columns, table, own_feats, own_aims = pl.pallas_call(
        early_kernel,
        out_shape=(
            jax.ShapeDtypeStruct((L, 128), jnp.int32),
            jax.ShapeDtypeStruct((8, 256), jnp.int32),
            jax.ShapeDtypeStruct((L, FEAT, M), bf16),
            jax.ShapeDtypeStruct((L, FEAT, M), bf16),
        ),
        in_specs=[in_vmem()] * 3,
        out_specs=(in_vmem(),) * 4,
        scratch_shapes=[pltpu.VMEM((L, 128), jnp.int32)],
        name="early",
        cost_estimate=pl.CostEstimate(flops=10**9, bytes_accessed=10**6, transcendentals=0),
    )(
        near_leaves,
        base_target.reshape(1, BLK_DEV),
        coords,
    )

    mine = pltpu.with_memory_space_constraint(mine, pltpu.VMEM)
    other = pltpu.with_memory_space_constraint(other, pltpu.VMEM)
    partial = pl.pallas_call(
        couple_kernel,
        out_shape=jax.ShapeDtypeStruct((NBASE, K, RHS), bf16),
        in_specs=[in_smem()] * 5 + [in_vmem()] * 4,
        out_specs=in_vmem(),
        scratch_shapes=[
            pltpu.VMEM((NBASE, MSG, RHS), bf16),
            pltpu.VMEM((NTOP, K, RHS), f32),
            pltpu.VMEM((NTOP, K, RHS), bf16),
            pltpu.VMEM((8 * BLK_DEV + 8, 128), f32),
            pltpu.VMEM((8 * TOPB_DEV, 128), f32),
            pltpu.SemaphoreType.DMA((2,)),
        ],
        name="couple",
        cost_estimate=pl.CostEstimate(flops=2 * 10**9, bytes_accessed=5 * 10**6, transcendentals=0),
    )(
        lax.axis_index(LEAF[3]).reshape(1).astype(jnp.int32),
        table,
        base_source,
        top_target,
        top_source,
        mine,
        other,
        base_coupling,
        top_coupling,
    )
    parts = lax.all_to_all(partial, LEAF, 0, 0, tiled=True)

    near_own = pl.pallas_call(
        own_kernel,
        out_shape=jax.ShapeDtypeStruct((L, M, RHS), f32),
        in_specs=[in_smem()] + [in_place()] * 3,
        out_specs=in_place(),
        scratch_shapes=[
            pltpu.VMEM((POINTS + M, RHS), bf16),
            pltpu.VMEM((L + 1, FEAT, M), bf16),
            pltpu.VMEM((L, FEAT, M), bf16),
            pltpu.VMEM((BATCH, M, OWN * M), bf16),
            pltpu.VMEM((BATCH, M, OWN * M), bf16),
            pltpu.VMEM((L, M, RHS), f32),
            pltpu.SemaphoreType.DMA((4,)),
        ],
        name="own",
        cost_estimate=pl.CostEstimate(
            flops=10**10, bytes_accessed=10**7, transcendentals=7 * 10**6
        ),
    )(columns, own_feats, own_aims, charges)
    near = pl.pallas_call(
        near_kernel,
        out_shape=jax.ShapeDtypeStruct((L, M, RHS), f32),
        in_specs=[in_smem()] * 2 + [in_place()] * 6,
        out_specs=in_place(),
        scratch_shapes=[
            pltpu.VMEM((3 * POINTS + M, RHS), bf16),
            pltpu.VMEM((3 * L + 1, FEAT, M), bf16),
            pltpu.VMEM((L, FEAT, M), bf16),
            pltpu.VMEM((2, TAIL, M), bf16),
            pltpu.VMEM((2, 3 * L, M), f32),
            pltpu.VMEM((M, REST * M), bf16),
            pltpu.VMEM((M, REST * M), bf16),
            pltpu.VMEM((UNITS, M, 2 * M), bf16),
            pltpu.VMEM((UNITS, M, 2 * M), bf16),
            pltpu.VMEM((L, M, RHS), f32),
            pltpu.SemaphoreType.DMA((9,)),
        ],
        name="near",
        cost_estimate=pl.CostEstimate(
            flops=4 * 10**10, bytes_accessed=10**7, transcendentals=3 * 10**7
        ),
    )(columns, table, own_feats, own_aims, before, charges, after, near_own)

    potential = pl.pallas_call(
        down_kernel,
        out_shape=jax.ShapeDtypeStruct((L, M, RHS), bf16),
        in_specs=[in_vmem()] + [in_place()] * 2,
        out_specs=in_place(),
        scratch_shapes=[
            pltpu.VMEM((L // 4, M, 4 * K), bf16),
            pltpu.VMEM((L, M, RHS), f32),
            pltpu.VMEM((L, M, RHS), bf16),
            pltpu.SemaphoreType.DMA((18,)),
        ],
        name="down",
        cost_estimate=pl.CostEstimate(flops=10**9, bytes_accessed=10**7, transcendentals=0),
    )(pltpu.with_memory_space_constraint(parts, pltpu.VMEM), v_rows, near)
    return potential.reshape(L * M, RHS)


def solution(mesh):
    split = Mesh(mesh.devices.reshape(4, 4, 4, 2), LEAF)
    by_leaf = P(LEAF, None)
    in_specs = (P(None, LEAF),) + (by_leaf,) * 8 + (P(LEAF), by_leaf, P(LEAF), P(LEAF))
    return jax.shard_map(
        all_steps, mesh=split, in_specs=in_specs, out_specs=by_leaf, check_vma=False
    )
```
